32 devices in a mesh: parts: 2 (over y), expert: 4 (over z), tensor: 4 (over x, core).
Axes of the slice: x: 2, y: 2, z: 4, core: 2. Of those that a mesh axis runs over, the one named last changes fastest.
Arguments:
- tokens: bfloat16 [128, 6144], P(('parts', 'expert'), 'tensor'), parts along dimension 0, may hold values from -4 to 4
- queries: bfloat16 [128, 48, 128], P(('parts', 'expert'), 'tensor'), parts along dimension 0, may hold values from -6 to 6
- new_kv: bfloat16 [2, 128, 8, 128], P(None, ('parts', 'expert'), 'tensor'), parts along dimension 1, may hold values from -6 to 6
- cache_kv: bfloat16 [2, 128, 16, 8, 128], P(None, ('parts', 'expert'), None, 'tensor'), parts along dimension 1, may hold values from -6 to 6
- lengths: int32 [128], P(('parts', 'expert')), parts along dimension 0, may hold values from 2 to 16
- gain: float32 [6144], P('tensor'), may hold values from 0.1 to 1.9
- gate_weight: bfloat16 [6144, 32768], P('tensor', 'expert'), may hold values from -0.078125 to 0.078125
- up_weight: bfloat16 [6144, 32768], P('tensor', 'expert'), may hold values from -0.078125 to 0.078125
- down_weight: bfloat16 [32768, 6144], P('expert', 'tensor'), may hold values from -0.0625 to 0.0625
- routes: int32 [128, 2], P(('parts', 'expert')), parts along dimension 0, may hold values from 0 to 3, all different within a row; in each aligned block of 16 rows (0 to 15, 16 to 31, ...) at most 9 rows name the same one
- route_weights: bfloat16 [128, 2], P(('parts', 'expert')), parts along dimension 0, may hold values from 0.19921875 to 0.796875
Outputs:
- mixed: bfloat16 [128, 6144], P(('parts', 'expert'), 'tensor'), parts along dimension 0
The draws below stay inside these ranges and needn't reach their ends.
There are 2 independent parts, one for each index of `parts`. The reference program is written for one: setup_inputs(seed, part) draws one part's arguments, and reference() takes and returns one part's arrays. A program takes and returns all parts, laid end to end along the dimension named above; an argument that names none is the same for every part. Nothing has to cross between parts.
Inputs may be any that keep to these rules, and one draw needn't show every extreme that they name: `routes`: the two entries of a row differ; in the rows of one index of expert no expert is named more than 9 times, a bound that some block reaches there in every draw.
All inputs are finite; a program needn't handle non-finite values.
Results may differ from the reference program's by a relative error of at most 0.0094.
Values may be sent and summed in bfloat16 or wider, within the bound.
A program may use at most 128 MiB of HBM per device.

```python
import math
import jax
import jax.numpy as jnp
import numpy as np
from jax import lax

D = 6144
QH = 48
KVH = 8
HD = 128
EXPERTS = 4
FF = 8192
CTX = 16
SEQ_DEV = 16
CAP = 9
TOKENS = 64


def draw_tokens(key, part):
    folded = jax.random.fold_in(key, 11)
    key_entries, key_rough, key_rows = jax.random.split(folded, 3)
    rising = jnp.exp(math.log(3.0) * jnp.arange(D, dtype=jnp.float32) / D)
    roughness = jnp.exp(jax.random.uniform(key_rough, (D,), jnp.float32, math.log(0.6), math.log(1.8)))
    columns = rising * roughness
    entries = jnp.clip(jax.random.normal(key_entries, (TOKENS, D), jnp.float32), -3.0, 3.0)
    scales = jnp.exp(jax.random.uniform(key_rows, (TOKENS, 1), jnp.float32, math.log(0.05), math.log(0.5)))
    return jnp.clip(entries * scales * columns, -4.0, 4.0).astype(jnp.bfloat16)


def draw_queries(key, part):
    key_query = jax.random.fold_in(key, 21)
    return jnp.clip(jax.random.normal(key_query, (TOKENS, QH, HD), jnp.float32), -6.0, 6.0).astype(jnp.bfloat16)


def draw_cache_kv(key, part):
    key_cache = jax.random.fold_in(key, 33)
    return jnp.clip(jax.random.normal(key_cache, (2, TOKENS, CTX, KVH, HD), jnp.float32), -6.0, 6.0).astype(jnp.bfloat16)


def set_ends(array, key, least, high):
    index_at = [jax.random.randint(jax.random.fold_in(key, axis), (), 0, length) for axis, length in enumerate(array.shape)]
    main_axis = array.shape.index(max(array.shape))
    beside = index_at[:main_axis] + [(index_at[main_axis] + 1) % array.shape[main_axis]] + index_at[main_axis + 1:]
    return array.at[tuple(index_at)].set(least).at[tuple(beside)].set(high)


def steps_of(key, extent, pieces, low, high):
    loudness, own = 1.0, jax.random.fold_in(key, 6)
    for dim, parts in pieces:
        draws = jnp.exp(jax.random.uniform(jax.random.fold_in(own, dim), (parts,), jnp.float32, low / len(pieces), high / len(pieces)))
        loudness = loudness * jnp.repeat(draws, extent[dim] // parts).reshape([-1 if axis == dim else 1 for axis in range(len(extent))])
    return loudness


def assign_block(key, own, number, rows, number_of, top, most, lean):
    order = jax.random.permutation(key, number_of)
    packed, common = load_shares(number_of, rows * top, most, lean, True), load_shares(number_of, rows * top, most, lean, False)
    places = jnp.arange(number_of)

    def named(sizes, turn):
        used = int((sizes > 0).sum())
        fixed = max(1, used // 4)
        moved = fixed + (places - fixed + turn * (used - fixed)) % max(1, number_of - fixed)
        return jnp.zeros((number_of,), jnp.int32).at[order[jnp.where(places < fixed, places, moved)]].set(jnp.asarray(sizes, jnp.int32))

    sizes = jnp.where(number % 4 == 0, named(packed, number // 4), named(common, number - number // 4 - 1))
    mixed = jax.random.permutation(jax.random.fold_in(own, 3), number_of)
    giver, receiver = mixed[0:number_of // 2 * 2:2], mixed[1:number_of // 2 * 2:2]
    margin = jnp.minimum(sizes[giver] - 1, most - sizes[receiver]) // 2
    margin = jnp.where((giver == order[0]) | (receiver == order[0]) | (sizes[receiver] == 0), 0, jnp.maximum(margin, 0))
    moved = jax.random.randint(jax.random.fold_in(own, 4), (number_of // 2,), 0, 1 << 20) % (margin + 1)
    sizes = sizes.at[giver].add(-moved).at[receiver].add(moved)
    items = jnp.searchsorted(jnp.cumsum(sizes), jnp.arange(rows * top), side="right").astype(jnp.int32)
    table = items.reshape(top, rows).T
    table = table[jax.random.permutation(jax.random.fold_in(own, 1), rows)]
    turn = jax.random.randint(jax.random.fold_in(own, 2), (rows, 1), 0, top)
    return jnp.take_along_axis(table, (jnp.arange(top)[None, :] + turn) % top, axis=1)


def load_shares(count, total, reach, lean, full):
    portions = [(1 << 20) // math.isqrt(grade ** lean) + 1 for grade in range(1, count + 1)]
    largest = reach if full else min(reach, max(-(-total // count), total * portions[0] // sum(portions)))
    least = 1 if total - largest >= count - 1 else 0
    counts, rest = [largest] + [least] * (count - 1), total - largest - least * (count - 1)
    while rest > 0:
        candidates = [i for i in range(1, count) if counts[i] < largest] or [i for i in range(1, count) if counts[i] < reach]
        pool, left = sum([portions[i] for i in candidates]), rest
        for i in candidates:
            addition = min(reach - counts[i], max(1, left * portions[i] // pool), rest)
            counts[i] = counts[i] + addition
            rest = rest - addition
    return np.array(counts)


def scatter_about(own_key, dims, scale, bound, shards=(), kind=jnp.bfloat16):
    loudness = steps_of(own_key, dims, shards, -0.22, 0.18) if shards else 1.0
    values = jax.random.normal(own_key, dims, jnp.float32) * scale * loudness
    return jnp.minimum(jnp.maximum(values, -bound), bound).astype(kind)


def setup_inputs(seed: int = 0, part: int = 0) -> dict:
    key_of = jax.random.split(jax.random.key(seed), 12)
    part_keys = jax.random.split(jax.random.fold_in(key_of[11], part), 12)
    tokens = draw_tokens(jax.random.fold_in(jax.random.fold_in(key_of[11], part), 71), part)
    queries = draw_queries(jax.random.fold_in(jax.random.fold_in(key_of[11], part), 71), part)
    new_kv = scatter_about(part_keys[2], (2, TOKENS, KVH, HD), 1.0, 6.0, ((1, 4), (2, 4)))
    cache_kv = draw_cache_kv(jax.random.fold_in(jax.random.fold_in(key_of[11], part), 71), part)
    lengths = set_ends(jax.random.randint(part_keys[4], (TOKENS,), 2, CTX + 1), jax.random.fold_in(part_keys[4], 1), 2, CTX).astype(jnp.int32)
    gain = jnp.clip(1.0 + 0.18 * jax.random.normal(key_of[5], (D,), jnp.float32), 0.1, 1.9)
    gate_weight = scatter_about(key_of[6], (D, EXPERTS * FF), D ** -0.5, 0.078125, ((0, 4), (1, 4)))
    up_weight = scatter_about(key_of[7], (D, EXPERTS * FF), D ** -0.5, 0.078125, ((0, 4), (1, 4)))
    down_weight = scatter_about(key_of[8], (EXPERTS * FF, D), FF ** -0.5, 0.0625, ((0, 4), (1, 4)))
    routes_keys = jax.random.split(jax.random.fold_in(part_keys[9], 1), TOKENS // SEQ_DEV)
    routes_turns = jax.random.permutation(jax.random.fold_in(part_keys[9], 3), TOKENS // SEQ_DEV)
    routes = jax.vmap(lambda own, number: assign_block(jax.random.fold_in(part_keys[9], 2), own, number, SEQ_DEV, EXPERTS, 2, CAP, 2))(routes_keys, routes_turns).reshape((TOKENS, 2))
    route_weights = jnp.clip(0.19921875 + 0.59765625 * jax.random.uniform(part_keys[10], (TOKENS, 2), jnp.float32) ** steps_of(part_keys[10], (TOKENS, 2), ((0, 4),), -0.2, 0.2), 0.19921875, 0.796875).astype(jnp.bfloat16)
    return {"tokens": tokens, "queries": queries, "new_kv": new_kv, "cache_kv": cache_kv, "lengths": lengths, "gain": gain, "gate_weight": gate_weight, "up_weight": up_weight, "down_weight": down_weight, "routes": routes, "route_weights": route_weights}


EPSILON = 1e-05

def attend(queries, new_kv, cache_kv, lengths):
    groups = QH // KVH
    sequences = queries.shape[0]
    factor = 1.0 / math.sqrt(HD)
    query_grp = queries.astype(jnp.float32).reshape(sequences, KVH, groups, HD)
    key_old = cache_kv[0].astype(jnp.float32)
    value_old = cache_kv[1].astype(jnp.float32)
    key_new = new_kv[0].astype(jnp.float32)
    value_new = new_kv[1].astype(jnp.float32)
    score_old = jnp.einsum('skgd,spkd->skgp', query_grp, key_old) * factor
    score_new = jnp.einsum('skgd,skd->skg', query_grp, key_new) * factor
    position = jnp.arange(key_old.shape[1], dtype=jnp.int32)
    usable = (position[None, :] < lengths[:, None])[:, None, None, :]
    score_old = jnp.where(usable, score_old, -jnp.inf)
    largest = jnp.maximum(lax.optimization_barrier(jnp.max(score_old, axis=3)), score_new)
    weight_old = jnp.exp(score_old - largest[..., None])
    weight_new = jnp.exp(score_new - largest)
    denominator = lax.optimization_barrier(jnp.sum(weight_old, axis=3)) + weight_new
    prob_old = lax.optimization_barrier((weight_old / denominator[..., None]).astype(jnp.bfloat16))
    prob_new = lax.optimization_barrier((weight_new / denominator).astype(jnp.bfloat16))
    attended = jnp.einsum('skgp,spkd->skgd', prob_old.astype(jnp.float32), value_old)
    attended = attended + prob_new.astype(jnp.float32)[..., None] * value_new[:, :, None, :]
    return attended.reshape(sequences, KVH * groups * HD)

def reference(tokens, queries, new_kv, cache_kv, lengths, gain, gate_weight, up_weight, down_weight, routes, route_weights):
    residual = tokens.astype(jnp.float32) + attend(queries, new_kv, cache_kv, lengths)
    row_ss = lax.optimization_barrier(jnp.sum(residual * residual, axis=1))
    normed = (residual * lax.rsqrt(row_ss[:, None] / D + EPSILON) * gain).astype(jnp.bfloat16)
    moe_sum = jnp.zeros(residual.shape, jnp.float32)
    for expert in range(EXPERTS):
        first = expert * FF
        gate_sum = jnp.dot(normed, gate_weight[:, first:first + FF], preferred_element_type=jnp.float32)
        lift_sum = jnp.dot(normed, up_weight[:, first:first + FF], preferred_element_type=jnp.float32)
        hidden = (jax.nn.silu(gate_sum) * lift_sum).astype(jnp.bfloat16)
        produced = jnp.dot(hidden, down_weight[first:first + FF, :], preferred_element_type=jnp.float32)
        share = lax.optimization_barrier(jnp.sum(jnp.where(routes == expert, route_weights.astype(jnp.float32), jnp.float32(0.0)), axis=1))
        moe_sum = moe_sum + share[:, None] * produced
    return (residual + moe_sum).astype(jnp.bfloat16)
```

```python
import functools
import math

import jax
import jax.numpy as jnp
from jax import lax
from jax.experimental import pallas as pl
from jax.experimental.pallas import tpu as pltpu
from jax.sharding import PartitionSpec as P

EXPERTS = 4
CAP = 9


EPSILON = 1e-05


def attend(queries, new_kv, cache_kv, lengths):
    sequences, head_count, head_size = queries.shape
    key_heads = new_kv.shape[2]
    groups = head_count // key_heads
    factor = 1.0 / math.sqrt(head_size)
    query_grp = queries.reshape(sequences, key_heads, groups, head_size)
    score_old = (
        jnp.einsum("skgd,spkd->skgp", query_grp, cache_kv[0], preferred_element_type=jnp.float32)
        * factor
    )
    score_new = (
        jnp.einsum("skgd,skd->skg", query_grp, new_kv[0], preferred_element_type=jnp.float32)
        * factor
    )
    position = jnp.arange(cache_kv.shape[2], dtype=jnp.int32)
    usable = (position[None, :] < lengths[:, None])[:, None, None, :]
    score_old = jnp.where(usable, score_old, -jnp.inf)
    largest = jnp.maximum(jnp.max(score_old, axis=3), score_new)
    weight_old = jnp.exp(score_old - largest[..., None])
    weight_new = jnp.exp(score_new - largest)
    denominator = jnp.sum(weight_old, axis=3) + weight_new
    prob_old = (weight_old / denominator[..., None]).astype(jnp.bfloat16)
    prob_new = (weight_new / denominator).astype(jnp.bfloat16)
    attended = jnp.einsum(
        "skgp,spkd->skgd", prob_old, cache_kv[1], preferred_element_type=jnp.float32
    )
    attended = (
        attended
        + prob_new.astype(jnp.float32)[..., None] * new_kv[1].astype(jnp.float32)[:, :, None, :]
    )
    return attended.reshape(sequences, head_count * head_size)


def expert_hidden(token_rows, gate_weight, up_weight, down_weight):
    gate_sum = jnp.dot(token_rows, gate_weight, preferred_element_type=jnp.float32)
    lift_sum = jnp.dot(token_rows, up_weight, preferred_element_type=jnp.float32)
    gate_sum, lift_sum = (
        lax.psum_scatter(gate_sum, "tensor", scatter_dimension=1, tiled=True),
        lax.psum_scatter(lift_sum, "tensor", scatter_dimension=1, tiled=True),
    )
    hidden = (jax.nn.silu(gate_sum) * lift_sum).astype(jnp.bfloat16)
    hidden = lax.all_gather(hidden, "tensor", axis=1, tiled=True)
    return jnp.dot(hidden, down_weight, preferred_element_type=jnp.float32)


def pack_slots(target, normed):
    slot_ids = jnp.arange(EXPERTS * CAP, dtype=jnp.int32)
    placing = (slot_ids[:, None, None] == target[None, :, :]).astype(jnp.float32)
    placing = jnp.sum(placing, axis=2).astype(jnp.bfloat16)
    packed = jnp.dot(placing, normed, preferred_element_type=jnp.float32).astype(jnp.bfloat16)
    return packed.reshape(EXPERTS, CAP, normed.shape[1])


def mix_slots(target, route_weights, per_slot):
    slot_ids = jnp.arange(EXPERTS * CAP, dtype=jnp.int32)
    mixing = jnp.where(
        slot_ids[None, None, :] == target[:, :, None],
        route_weights.astype(jnp.float32)[:, :, None],
        jnp.float32(0.0),
    )
    mixing = jnp.sum(mixing, axis=1)
    return jnp.dot(
        mixing, per_slot, precision=lax.Precision.HIGHEST, preferred_element_type=jnp.float32
    )


def on_device(
    tokens,
    queries,
    new_kv,
    cache_kv,
    lengths,
    gain,
    gate_weight,
    up_weight,
    down_weight,
    routes,
    route_weights,
):
    local_seqs, local_width = tokens.shape
    residual = tokens.astype(jnp.float32) + attend(queries, new_kv, cache_kv, lengths)
    full_width = local_width * lax.axis_size("tensor")
    squares = lax.psum(jnp.sum(residual * residual, axis=1), "tensor")
    normed = (residual * lax.rsqrt(squares[:, None] / full_width + EPSILON) * gain).astype(
        jnp.bfloat16
    )
    choosers = (routes[:, :, None] == jnp.arange(EXPERTS, dtype=jnp.int32)[None, None, :]).astype(
        jnp.int32
    )
    flat_choice = choosers.reshape(2 * local_seqs, EXPERTS)
    earlier = jnp.cumsum(flat_choice, axis=0) - flat_choice
    slot_index = jnp.sum(earlier * flat_choice, axis=1)
    target = (routes.reshape(-1) * CAP + slot_index).reshape(local_seqs, 2)
    devices = lax.axis_size("expert")
    per_expert = devices // EXPERTS
    packed = pack_slots(target, normed).reshape(EXPERTS, 1, CAP, local_width)
    outgoing = jnp.broadcast_to(packed, (EXPERTS, per_expert, CAP, local_width)).reshape(
        devices, CAP, local_width
    )
    arrived = lax.all_to_all(outgoing, "expert", split_axis=0, concat_axis=0, tiled=True)
    sources = arrived.shape[0]
    items = arrived.shape[1]
    produced = expert_hidden(
        arrived.reshape(sources * items, local_width), gate_weight, up_weight, down_weight
    )
    computed = produced.reshape(sources, items, local_width)
    returned = lax.all_to_all(computed, "expert", split_axis=0, concat_axis=0, tiled=True)
    per_slot = jnp.sum(returned.reshape(EXPERTS, per_expert, CAP, local_width), axis=1)
    moe_sum = mix_slots(target, route_weights, per_slot.reshape(EXPERTS * CAP, local_width))
    return (residual + moe_sum).astype(jnp.bfloat16)


MESH = pl.DeviceIdType.MESH


def fused_kernel(
    dims,
    lengths_hbm, routes_hbm,
    tokens_hbm, queries_hbm, new_hbm, cache_hbm, gain_hbm, mixw_hbm,
    gate_hbm, up_hbm, down_hbm,
    out_ref,
    lens, route, tok, qry, new, cache, gain, mixw, resid, mixt,
    ysend, arr, ss_rows, flat, tall, xin,
    gate_w, up_w, down_w,
    part, got1, half16, half32, got2, hid, acc, rtall, ret_send, ret,
    in_sem, gate_sem, up_sem, down_sem,
    a2a_send, a2a_recv, sr_send, sr_recv,
    s1_send, s1_recv, s2_send, s2_recv, h1_send, h1_recv, h2_send, h2_recv, h3_send, h3_recv,
    rt_send, rt_recv,
):
    seqs, heads, groups, hd, ctx, kvh, full_width, chunks, width, slots, rows, blocks = dims
    half, quarter = width // 2, width // 4
    p = lax.axis_index("parts")
    me = lax.axis_index("expert")
    t = lax.axis_index("tensor")
    core = lax.rem(t, 2)
    xpos = lax.div(t, 2)
    sibling = t + 1 - 2 * core
    across = lax.rem(t + 2, 4)
    diagonal = lax.rem(sibling + 2, 4)
    f32, bf16 = jnp.float32, jnp.bfloat16

    barrier = pltpu.get_barrier_semaphore()
    for j in range(1, EXPERTS):
        pl.semaphore_signal(barrier, inc=1, device_id=(p, lax.rem(me + j, EXPERTS), t), device_id_type=MESH)
    for other in (sibling, across, diagonal):
        pl.semaphore_signal(barrier, inc=1, device_id=(p, me, other), device_id_type=MESH)

    small = [
        pltpu.make_async_copy(a, b, in_sem.at[n])
        for n, (a, b) in enumerate(
            [
                (queries_hbm, qry), (cache_hbm, cache), (new_hbm, new), (lengths_hbm, lens), (routes_hbm, route),
                (tokens_hbm, tok), (gain_hbm, gain), (mixw_hbm, mixw),
            ]
        )
    ]
    for cp in small:
        cp.start()

    def gate_copy(i):
        s = lax.rem(i, slots)
        cols = pl.ds(pl.multiple_of(i * width, width), width)
        return pltpu.make_async_copy(gate_hbm.at[:, cols], gate_w.at[s], gate_sem.at[s])

    def up_copy(i):
        s = lax.rem(i, slots)
        cols = pl.ds(pl.multiple_of(i * width, width), width)
        return pltpu.make_async_copy(up_hbm.at[:, cols], up_w.at[s], up_sem.at[s])

    def down_copy(i):
        rws = pl.ds(pl.multiple_of(i * width, width), width)
        return pltpu.make_async_copy(down_hbm.at[rws, :], down_w.at[i], down_sem.at[i])

    for i in range(2):
        gate_copy(i).start(priority=1)
        up_copy(i).start(priority=1)
    tall[...] = jnp.zeros_like(tall)
    rtall[...] = jnp.zeros_like(rtall)
    acc[...] = jnp.zeros_like(acc)
    for cp in small:
        cp.wait()

    prow = lax.broadcasted_iota(jnp.int32, (rows, seqs), 0)
    expert_of = sum((prow >= e * CAP).astype(jnp.int32) for e in range(1, EXPERTS + 1))
    picks = [route[j : j + 1, :] == expert_of for j in range(2)]
    named = jnp.where(picks[0] | picks[1], f32(1.0), f32(0.0))
    earlier = lax.broadcasted_iota(jnp.int32, (seqs, seqs), 0) < lax.broadcasted_iota(jnp.int32, (seqs, seqs), 1)
    before = jnp.dot(
        named.astype(bf16), jnp.where(earlier, f32(1.0), f32(0.0)).astype(bf16), preferred_element_type=f32
    )
    slot_of = (prow - expert_of * CAP).astype(f32)
    placing = jnp.where(before == slot_of, named, f32(0.0))
    weights = mixw[...].astype(f32)
    mixing = placing * jnp.where(picks[0], weights[0:1], weights[1:2])
    same = lax.broadcasted_iota(jnp.int32, (seqs, seqs), 0) == lax.broadcasted_iota(jnp.int32, (seqs, seqs), 1)
    mixt[...] = lax.dot_general(
        jnp.where(same, f32(1.0), f32(0.0)).astype(bf16), mixing.astype(bf16), (((1,), (1,)), ((), ())),
        preferred_element_type=f32,
    ).astype(bf16)
    q = qry[...].reshape(heads * seqs, hd)
    factor = 1.0 / math.sqrt(hd)
    dn = (((1,), (1,)), ((), ()))
    nq, nk, nn = heads * seqs, seqs * ctx * kvh, seqs * kvh
    s_old = lax.dot_general(q, cache[0], dn, preferred_element_type=f32) * factor
    s_new = lax.dot_general(q, new[0], dn, preferred_element_type=f32) * factor
    kcol = lax.broadcasted_iota(jnp.int32, (1, nk), 1)
    owner = lax.broadcasted_iota(jnp.int32, (seqs, nk), 0)
    spread = lax.broadcasted_iota(jnp.int32, (seqs, nk), 1) // (ctx * kvh) == owner
    limit = jnp.dot(
        lens[...].astype(f32).astype(bf16), jnp.where(spread, f32(1.0), f32(0.0)).astype(bf16),
        preferred_element_type=f32,
    )
    kpos = (kcol // kvh) % ctx
    key_old = jnp.where(kpos.astype(f32) < limit, (kcol // (ctx * kvh)) * kvh + kcol % kvh, -1)
    key_new = lax.broadcasted_iota(jnp.int32, (1, nn), 1)
    qrow = lax.broadcasted_iota(jnp.int32, (nq, 1), 0)
    key_q = (qrow % seqs) * kvh + qrow // (seqs * groups)
    low = f32(-1e30)
    s_old = jnp.where(key_q == key_old, s_old, low)
    s_new = jnp.where(key_q == key_new, s_new, low)
    largest = jnp.maximum(jnp.max(s_old, axis=1, keepdims=True), jnp.max(s_new, axis=1, keepdims=True))
    w_old = jnp.exp(s_old - largest)
    w_new = jnp.exp(s_new - largest)
    den = jnp.sum(w_old, axis=1, keepdims=True) + jnp.sum(w_new, axis=1, keepdims=True)
    p_old = (w_old / den).astype(bf16)
    p_new = (w_new / den).astype(bf16)
    att = jnp.dot(p_old, cache[1], preferred_element_type=f32) + jnp.dot(
        p_new, new[1], preferred_element_type=f32
    )
    for h in range(heads):
        cols = slice(h * hd, (h + 1) * hd)
        piece = tok[:, cols].astype(f32) + att[h * seqs : (h + 1) * seqs]
        resid[:, cols] = piece
    scaled = (resid[...] * gain[...].reshape(1, -1)).astype(bf16)
    flat[...] = jnp.dot(placing.astype(bf16), scaled, preferred_element_type=f32)
    fold(flat, tall, ysend)
    for i in range(2, slots):
        gate_copy(i).start(priority=1)
        up_copy(i).start(priority=1)
    pl.semaphore_wait(barrier, EXPERTS + 2)

    def exchange(src, dst, send, recv, j):
        to = lax.rem(me + j, EXPERTS)
        return pltpu.make_async_remote_copy(
            src_ref=src.at[to], dst_ref=dst.at[me], send_sem=send.at[j - 1], recv_sem=recv.at[j - 1],
            device_id=(p, to, t), device_id_type=MESH,
        )

    for j in (2, 3, 1):
        exchange(ysend, arr, a2a_send, a2a_recv, j).start()
    arr[me] = ysend[me]
    for j in (1, 2, 3):
        exchange(ysend, arr, a2a_send, a2a_recv, j).wait()
    unfold(arr, tall, flat)
    xin[...] = flat[...].astype(bf16)

    def ss_copy(j):
        return pltpu.make_async_remote_copy(
            src_ref=ss_rows.at[t], dst_ref=ss_rows.at[t], send_sem=sr_send.at[j - 1], recv_sem=sr_recv.at[j - 1],
            device_id=(p, me, lax.rem(t + j, 4)), device_id_type=MESH,
        )

    def remote(src, dst, send, recv, i, to):
        return pltpu.make_async_remote_copy(
            src_ref=src, dst_ref=dst, send_sem=send.at[i], recv_sem=recv.at[i],
            device_id=(p, me, to), device_id_type=MESH,
        )

    def at_half(c):
        return pl.ds(pl.multiple_of(c * half, half), half)

    def at_quarter(n):
        return pl.ds(pl.multiple_of(n * quarter, quarter), quarter)

    mine = core * 2 + xpos
    theirs = core * 2 + 1 - xpos

    def stage1(i):
        return remote(part.at[i, :, :, at_half(1 - core)], got1.at[i], s1_send, s1_recv, i, sibling)

    def stage2(i):
        return remote(half16.at[i, :, :, at_quarter(1 - xpos)], got2.at[i], s2_send, s2_recv, i, across)

    def spread1(i):
        return remote(hid.at[i, :, at_quarter(mine)], hid.at[i, :, at_quarter(mine)], h1_send, h1_recv, i, across)

    def spread2(i):
        return remote(hid.at[i, :, at_quarter(mine)], hid.at[i, :, at_quarter(mine)], h2_send, h2_recv, i, sibling)

    def spread3(i):
        return remote(hid.at[i, :, at_quarter(theirs)], hid.at[i, :, at_quarter(theirs)], h3_send, h3_recv, i, sibling)

    def exchange_squares():
        raw = flat[...] * (1.0 / gain[...].reshape(1, -1))
        ss_rows[t] = jnp.broadcast_to(jnp.sum(raw * raw, axis=1, keepdims=True), (rows, 128))
        for j in (1, 2, 3):
            ss_copy(j).start()

    def direct(i):
        return remote(hid.at[i, :, at_quarter(mine)], hid.at[i, :, at_quarter(mine)], h3_send, h3_recv, i, diagonal)

    def multiply(i):
        s = lax.rem(i, slots)
        gate_copy(i).wait()
        part[i, 0] = jnp.dot(xin[...], gate_w[s], preferred_element_type=f32).astype(bf16)
        up_copy(i).wait()
        part[i, 1] = jnp.dot(xin[...], up_w[s], preferred_element_type=f32).astype(bf16)
        stage1(i).start()
        pl.when(i == 0)(exchange_squares)

        @pl.when(i + slots < chunks)
        def _():
            gate_copy(i + slots).start(priority=1)
            up_copy(i + slots).start(priority=1)

        for n in (2 * (i - chunks + slots) - 1, 2 * (i - chunks + slots)):
            pl.when((n >= 0) & (n < chunks))(lambda n=n: down_copy(n).start(priority=1))

    def add_core(b):
        stage1(b).wait_recv()
        for n in range(2):
            both = part[b, n, :, at_half(core)].astype(f32) + got1[b, n].astype(f32)
            half32[b, n] = both
            half16[b, n] = both.astype(bf16)
        stage2(b).start()

    def activate(c):
        @pl.when(c == 0)
        def _():
            for j in (1, 2, 3):
                ss_copy(j).wait()
            ss_rows[t] = ss_rows[0] + ss_rows[1] + ss_rows[2] + ss_rows[3]

        stage2(c).wait_recv()
        scale = lax.rsqrt(ss_rows[t][:, :1] / full_width + EPSILON)
        g = (half32[c, 0, :, at_quarter(xpos)] + got2[c, 0].astype(f32)) * scale
        u = (half32[c, 1, :, at_quarter(xpos)] + got2[c, 1].astype(f32)) * scale
        hid[c, :, at_quarter(mine)] = (g / (1.0 + jnp.exp(-g)) * u).astype(bf16)
        spread1(c).start()
        spread2(c).start()

        @pl.when(c >= chunks - DIRECT)
        def _():
            direct(c).start()

    def hand_on(d):
        @pl.when(d < chunks - DIRECT)
        def _():
            spread1(d).wait_recv()
            spread3(d).start()

    def ready(e):
        @pl.when(e >= chunks - DIRECT)
        def _():
            spread1(e).wait_recv()

        spread2(e).wait_recv()
        spread3(e).wait_recv()
        down_copy(e).wait()

    def project(e):
        ready(e)
        acc[...] += jnp.dot(hid[e], down_w[e], preferred_element_type=f32)

    def step(i, carry):
        multiply(i)
        pl.when(i >= 1)(lambda: add_core(i - 1))
        pl.when(i >= 3)(lambda: activate(i - 3))
        pl.when(i >= 5)(lambda: hand_on(i - 5))
        return carry

    lax.fori_loop(0, chunks, step, 0)

    def finish(u, carry):
        project(u)
        pl.when(u == 0)(lambda: add_core(u + chunks - 1))
        late = jnp.maximum(u - 1, 0)

        @pl.when((u == 0) | (u == 2) | (u == 3))
        def _():
            activate(late + chunks - 3)
            hand_on(late + chunks - 5)

        return carry

    lax.fori_loop(0, chunks - 1, finish, 0)

    def give(b, j):
        to = lax.rem(me + j, EXPERTS)
        return pltpu.make_async_remote_copy(
            src_ref=ret_send.at[b, to], dst_ref=ret.at[b, me], send_sem=rt_send.at[b, j - 1], recv_sem=rt_recv.at[b, j - 1],
            device_id=(p, to, t), device_id_type=MESH,
        )

    last = chunks - 1
    wide = acc.shape[1] // blocks
    ready(last)
    for b in range(blocks):
        cols = slice(b * wide, (b + 1) * wide)
        acc[:, cols] += jnp.dot(hid[last], down_w[last, :, cols], preferred_element_type=f32)
        fold(acc.at[:, cols], rtall, ret_send.at[b])
        for j in (2, 3, 1):
            give(b, j).start()
        ret[b, me] = ret_send[b, me]

    def drain(i, carry):
        for copy in (stage1, stage2, spread1, spread2, spread3):
            copy(i).wait_send()
        return carry

    lax.fori_loop(0, chunks, drain, 0)
    for b in range(blocks):
        cols = slice(b * wide, (b + 1) * wide)
        for j in (1, 2, 3):
            give(b, j).wait()
        unfold(ret.at[b], rtall, flat.at[:, cols])
        moe = jnp.dot(mixt[...], flat[:, cols].astype(bf16), preferred_element_type=f32)
        out_ref[:, cols] = (resid[:, cols] + moe).astype(bf16)


def fold(flat, tall, out):
    for e in range(EXPERTS):
        for j in range(flat.shape[1] // 128):
            tall[e, j * CAP : (j + 1) * CAP] = flat[e * CAP : (e + 1) * CAP, j * 128 : (j + 1) * 128]
        out[e] = tall[e].astype(out.dtype)


def unfold(src, tall, flat):
    for e in range(EXPERTS):
        tall[e] = src[e].astype(tall.dtype)
        for j in range(flat.shape[1] // 128):
            flat[e * CAP : (e + 1) * CAP, j * 128 : (j + 1) * 128] = tall[e, j * CAP : (j + 1) * CAP]


DIRECT = 2


def fused(
    tokens, queries, new_kv, cache_kv, lengths, gain, gate_weight, up_weight, down_weight, routes, route_weights
):
    seqs, width_in = tokens.shape
    heads, hd = queries.shape[1:]
    ctx, kvh = cache_kv.shape[2:4]
    ff = gate_weight.shape[1]
    width = min(1024, ff)
    chunks = ff // width
    slots = min(5, chunks)
    rows = -(-EXPERTS * CAP // 8) * 8
    full_width = width_in * lax.axis_size("tensor")
    blocks = 2
    dims = (seqs, heads, heads // kvh, hd, ctx, kvh, full_width, chunks, width, slots, rows, blocks)
    low = -(-(width_in // 128 // blocks * CAP) // 8) * 8
    high = -(-(width_in // 128 * CAP) // 16) * 16
    half, quarter = width // 2, width // 4
    bf16, f32 = jnp.bfloat16, jnp.float32
    vm, dma = pltpu.VMEM, pltpu.SemaphoreType.DMA
    nk, nn = seqs * ctx * kvh, seqs * kvh
    scratch = [
        vm((1, seqs), jnp.int32), vm((2, seqs), jnp.int32),
        vm((seqs, width_in), bf16), vm((heads, seqs, hd), bf16), vm((2, nn, hd), bf16), vm((2, nk, hd), bf16),
        vm((width_in,), f32), vm((2, seqs), bf16), vm((seqs, width_in), f32), vm((seqs, rows), bf16),
        vm((EXPERTS, high, 128), bf16), vm((EXPERTS, high, 128), bf16),
        vm((4, rows, 128), f32), vm((rows, width_in), f32), vm((EXPERTS, high, 128), f32),
        vm((rows, width_in), bf16),
        vm((slots, width_in, width), bf16), vm((slots, width_in, width), bf16), vm((chunks, width, width_in), bf16),
        vm((chunks, 2, rows, width), bf16), vm((chunks, 2, rows, half), bf16),
        vm((chunks, 2, rows, half), bf16), vm((chunks, 2, rows, half), f32),
        vm((chunks, 2, rows, quarter), bf16), vm((chunks, rows, width), bf16),
        vm((rows, width_in), f32), vm((EXPERTS, low, 128), f32),
        vm((blocks, EXPERTS, low, 128), bf16), vm((blocks, EXPERTS, low, 128), bf16),
        dma((8,)), dma((slots,)), dma((slots,)), dma((chunks,)),
    ] + [dma((3,))] * 4 + [dma((chunks,))] * 10 + [dma((blocks, 3))] * 2
    anyspace = pl.BlockSpec(memory_space=pl.ANY)
    return pl.pallas_call(
        functools.partial(fused_kernel, dims),
        out_shape=jax.ShapeDtypeStruct((seqs, width_in), bf16),
        in_specs=[anyspace] * 11,
        out_specs=pl.BlockSpec(memory_space=pltpu.VMEM),
        scratch_shapes=scratch,
        compiler_params=pltpu.CompilerParams(
            collective_id=0, has_side_effects=True, vmem_limit_bytes=67043328
        ),
    )(
        lengths.reshape(1, seqs), routes.T, tokens, jnp.transpose(queries, (1, 0, 2)), new_kv.reshape(2, nn, hd), cache_kv.reshape(2, nk, hd),
        gain, route_weights.T, gate_weight, up_weight, down_weight,
    )


def solution(mesh):
    in_specs = (
        P(("parts", "expert"), "tensor"),
        P(("parts", "expert"), "tensor", None),
        P(None, ("parts", "expert"), "tensor", None),
        P(None, ("parts", "expert"), None, "tensor", None),
        P(("parts", "expert")),
        P("tensor"),
        P("tensor", "expert"),
        P("tensor", "expert"),
        P("expert", "tensor"),
        P(("parts", "expert"), None),
        P(("parts", "expert"), None),
    )
    out_specs = P(("parts", "expert"), "tensor")
    square = mesh.shape["expert"] == EXPERTS and mesh.shape["tensor"] == 4

    def run(*args):
        wide = args[6].shape[1] >= 8 * 1024
        return (fused if square and wide else on_device)(*args)

    return jax.shard_map(
        run, mesh=mesh, in_specs=in_specs, out_specs=out_specs, check_vma=False
    )
```

```python
import functools
import math

import jax
import jax.numpy as jnp
from jax import lax
from jax.experimental import pallas as pl
from jax.experimental.pallas import tpu as pltpu
from jax.sharding import PartitionSpec as P

EXPERTS = 4
CAP = 9


EPSILON = 1e-05


def attend(queries, new_kv, cache_kv, lengths):
    sequences, head_count, head_size = queries.shape
    key_heads = new_kv.shape[2]
    groups = head_count // key_heads
    factor = 1.0 / math.sqrt(head_size)
    query_grp = queries.reshape(sequences, key_heads, groups, head_size)
    score_old = (
        jnp.einsum("skgd,spkd->skgp", query_grp, cache_kv[0], preferred_element_type=jnp.float32)
        * factor
    )
    score_new = (
        jnp.einsum("skgd,skd->skg", query_grp, new_kv[0], preferred_element_type=jnp.float32)
        * factor
    )
    position = jnp.arange(cache_kv.shape[2], dtype=jnp.int32)
    usable = (position[None, :] < lengths[:, None])[:, None, None, :]
    score_old = jnp.where(usable, score_old, -jnp.inf)
    largest = jnp.maximum(jnp.max(score_old, axis=3), score_new)
    weight_old = jnp.exp(score_old - largest[..., None])
    weight_new = jnp.exp(score_new - largest)
    denominator = jnp.sum(weight_old, axis=3) + weight_new
    prob_old = (weight_old / denominator[..., None]).astype(jnp.bfloat16)
    prob_new = (weight_new / denominator).astype(jnp.bfloat16)
    attended = jnp.einsum(
        "skgp,spkd->skgd", prob_old, cache_kv[1], preferred_element_type=jnp.float32
    )
    attended = (
        attended
        + prob_new.astype(jnp.float32)[..., None] * new_kv[1].astype(jnp.float32)[:, :, None, :]
    )
    return attended.reshape(sequences, head_count * head_size)


def expert_hidden(token_rows, gate_weight, up_weight, down_weight):
    gate_sum = jnp.dot(token_rows, gate_weight, preferred_element_type=jnp.float32)
    lift_sum = jnp.dot(token_rows, up_weight, preferred_element_type=jnp.float32)
    gate_sum, lift_sum = (
        lax.psum_scatter(gate_sum, "tensor", scatter_dimension=1, tiled=True),
        lax.psum_scatter(lift_sum, "tensor", scatter_dimension=1, tiled=True),
    )
    hidden = (jax.nn.silu(gate_sum) * lift_sum).astype(jnp.bfloat16)
    hidden = lax.all_gather(hidden, "tensor", axis=1, tiled=True)
    return jnp.dot(hidden, down_weight, preferred_element_type=jnp.float32)


def pack_slots(target, normed):
    slot_ids = jnp.arange(EXPERTS * CAP, dtype=jnp.int32)
    placing = (slot_ids[:, None, None] == target[None, :, :]).astype(jnp.float32)
    placing = jnp.sum(placing, axis=2).astype(jnp.bfloat16)
    packed = jnp.dot(placing, normed, preferred_element_type=jnp.float32).astype(jnp.bfloat16)
    return packed.reshape(EXPERTS, CAP, normed.shape[1])


def mix_slots(target, route_weights, per_slot):
    slot_ids = jnp.arange(EXPERTS * CAP, dtype=jnp.int32)
    mixing = jnp.where(
        slot_ids[None, None, :] == target[:, :, None],
        route_weights.astype(jnp.float32)[:, :, None],
        jnp.float32(0.0),
    )
    mixing = jnp.sum(mixing, axis=1)
    return jnp.dot(
        mixing, per_slot, precision=lax.Precision.HIGHEST, preferred_element_type=jnp.float32
    )


def on_device(
    tokens,
    queries,
    new_kv,
    cache_kv,
    lengths,
    gain,
    gate_weight,
    up_weight,
    down_weight,
    routes,
    route_weights,
):
    local_seqs, local_width = tokens.shape
    residual = tokens.astype(jnp.float32) + attend(queries, new_kv, cache_kv, lengths)
    full_width = local_width * lax.axis_size("tensor")
    squares = lax.psum(jnp.sum(residual * residual, axis=1), "tensor")
    normed = (residual * lax.rsqrt(squares[:, None] / full_width + EPSILON) * gain).astype(
        jnp.bfloat16
    )
    choosers = (routes[:, :, None] == jnp.arange(EXPERTS, dtype=jnp.int32)[None, None, :]).astype(
        jnp.int32
    )
    flat_choice = choosers.reshape(2 * local_seqs, EXPERTS)
    earlier = jnp.cumsum(flat_choice, axis=0) - flat_choice
    slot_index = jnp.sum(earlier * flat_choice, axis=1)
    target = (routes.reshape(-1) * CAP + slot_index).reshape(local_seqs, 2)
    devices = lax.axis_size("expert")
    per_expert = devices // EXPERTS
    packed = pack_slots(target, normed).reshape(EXPERTS, 1, CAP, local_width)
    outgoing = jnp.broadcast_to(packed, (EXPERTS, per_expert, CAP, local_width)).reshape(
        devices, CAP, local_width
    )
    arrived = lax.all_to_all(outgoing, "expert", split_axis=0, concat_axis=0, tiled=True)
    sources = arrived.shape[0]
    items = arrived.shape[1]
    produced = expert_hidden(
        arrived.reshape(sources * items, local_width), gate_weight, up_weight, down_weight
    )
    computed = produced.reshape(sources, items, local_width)
    returned = lax.all_to_all(computed, "expert", split_axis=0, concat_axis=0, tiled=True)
    per_slot = jnp.sum(returned.reshape(EXPERTS, per_expert, CAP, local_width), axis=1)
    moe_sum = mix_slots(target, route_weights, per_slot.reshape(EXPERTS * CAP, local_width))
    return (residual + moe_sum).astype(jnp.bfloat16)


MESH = pl.DeviceIdType.MESH


def fused_kernel(
    dims,
    lengths_hbm, routes_hbm,
    tokens_hbm, queries_hbm, new_hbm, cache_hbm, gain_hbm, mixw_hbm,
    gate_hbm, up_hbm, down_hbm,
    out_ref,
    lens, route, tok, qry, new, cache, gain, mixw, resid, mixt,
    ysend, arr, ss_rows, flat, tall,
    lift_w, down_w,
    part, got1, half16, half32, got2, hid, acc, rtall, ret_send, ret,
    in_sem, lift_sem, down_sem, sent, a2a_recv, sr_recv,
    s1_recv, s2_recv, h1_recv, h2_recv, rt_recv,
):
    seqs, heads, groups, hd, ctx, kvh, full_width, chunks, width, slots, rows, blocks = dims
    half, quarter = width // 2, width // 4
    p = lax.axis_index("parts")
    me = lax.axis_index("expert")
    t = lax.axis_index("tensor")
    core = lax.rem(t, 2)
    xpos = lax.div(t, 2)
    sibling = t + 1 - 2 * core
    partner = lax.rem(sibling + 2, 4)
    other = lax.rem(t + 2, 4)
    own = lax.rem(core + xpos, 2)
    f32, bf16 = jnp.float32, jnp.bfloat16

    barrier = pltpu.get_barrier_semaphore()
    for j in range(1, EXPERTS):
        pl.semaphore_signal(barrier, inc=1, device_id=(p, lax.rem(me + j, EXPERTS), t), device_id_type=MESH)
    for peer in (sibling, partner, other):
        pl.semaphore_signal(barrier, inc=1, device_id=(p, me, peer), device_id_type=MESH)

    small = [
        pltpu.make_async_copy(a, b, in_sem.at[n])
        for n, (a, b) in enumerate(
            [
                (queries_hbm, qry), (cache_hbm, cache), (new_hbm, new), (lengths_hbm, lens), (routes_hbm, route),
                (tokens_hbm, tok), (gain_hbm, gain), (mixw_hbm, mixw),
            ]
        )
    ]
    for cp in small:
        cp.start()

    def gate_copy(i):
        s = i % slots
        cols = pl.ds(i * width, width)
        return pltpu.make_async_copy(gate_hbm.at[:, cols], lift_w.at[s, 0], lift_sem.at[s])

    def up_copy(i):
        s = i % slots
        cols = pl.ds(i * width, width)
        return pltpu.make_async_copy(up_hbm.at[:, cols], lift_w.at[s, 1], lift_sem.at[s])

    def down_copy(i):
        rws = pl.ds(i * width, width)
        return pltpu.make_async_copy(down_hbm.at[rws, :], down_w.at[i], down_sem.at[i])

    for i in range(2):
        gate_copy(i).start(priority=1)
        up_copy(i).start(priority=1)
    tall[...] = jnp.zeros_like(tall)
    rtall[...] = jnp.zeros_like(rtall)
    acc[...] = jnp.zeros_like(acc)
    for cp in small:
        cp.wait()

    prow = lax.broadcasted_iota(jnp.int32, (rows, seqs), 0)
    expert_of = sum((prow >= e * CAP).astype(jnp.int32) for e in range(1, EXPERTS + 1))
    picks = [route[j : j + 1, :] == expert_of for j in range(2)]
    named = jnp.where(picks[0] | picks[1], f32(1.0), f32(0.0))
    earlier = lax.broadcasted_iota(jnp.int32, (seqs, seqs), 0) < lax.broadcasted_iota(jnp.int32, (seqs, seqs), 1)
    before = jnp.dot(
        named.astype(bf16), jnp.where(earlier, f32(1.0), f32(0.0)).astype(bf16), preferred_element_type=f32
    )
    slot_of = (prow - expert_of * CAP).astype(f32)
    placing = jnp.where(before == slot_of, named, f32(0.0))
    weights = mixw[...].astype(f32)
    mixing = placing * jnp.where(picks[0], weights[0:1], weights[1:2])
    same = lax.broadcasted_iota(jnp.int32, (seqs, seqs), 0) == lax.broadcasted_iota(jnp.int32, (seqs, seqs), 1)
    mixt[...] = lax.dot_general(
        jnp.where(same, f32(1.0), f32(0.0)).astype(bf16), mixing.astype(bf16), (((1,), (1,)), ((), ())),
        preferred_element_type=f32,
    ).astype(bf16)
    q = qry[...].reshape(heads * seqs, hd)
    factor = 1.0 / math.sqrt(hd)
    dn = (((1,), (1,)), ((), ()))
    nq, nk, nn = heads * seqs, seqs * ctx * kvh, seqs * kvh
    s_old = lax.dot_general(q, cache[0], dn, preferred_element_type=f32) * factor
    s_new = lax.dot_general(q, new[0], dn, preferred_element_type=f32) * factor
    kcol = lax.broadcasted_iota(jnp.int32, (1, nk), 1)
    owner = lax.broadcasted_iota(jnp.int32, (seqs, nk), 0)
    spread = lax.broadcasted_iota(jnp.int32, (seqs, nk), 1) // (ctx * kvh) == owner
    limit = jnp.dot(
        lens[...].astype(f32).astype(bf16), jnp.where(spread, f32(1.0), f32(0.0)).astype(bf16),
        preferred_element_type=f32,
    )
    kpos = (kcol // kvh) % ctx
    key_old = jnp.where(kpos.astype(f32) < limit, (kcol // (ctx * kvh)) * kvh + kcol % kvh, -1)
    key_new = lax.broadcasted_iota(jnp.int32, (1, nn), 1)
    qrow = lax.broadcasted_iota(jnp.int32, (nq, 1), 0)
    key_q = (qrow % seqs) * kvh + qrow // (seqs * groups)
    low = f32(-1e30)
    s_old = jnp.where(key_q == key_old, s_old, low)
    s_new = jnp.where(key_q == key_new, s_new, low)
    largest = jnp.maximum(jnp.max(s_old, axis=1, keepdims=True), jnp.max(s_new, axis=1, keepdims=True))
    w_old = jnp.exp(s_old - largest)
    w_new = jnp.exp(s_new - largest)
    den = jnp.sum(w_old, axis=1, keepdims=True) + jnp.sum(w_new, axis=1, keepdims=True)
    p_old = (w_old / den).astype(bf16)
    p_new = (w_new / den).astype(bf16)
    att = jnp.dot(p_old, cache[1], preferred_element_type=f32) + jnp.dot(
        p_new, new[1], preferred_element_type=f32
    )
    for h in range(heads):
        cols = slice(h * hd, (h + 1) * hd)
        piece = tok[:, cols].astype(f32) + att[h * seqs : (h + 1) * seqs]
        resid[:, cols] = piece
    scaled = (resid[...] * gain[...].reshape(1, -1)).astype(bf16)
    flat[...] = jnp.dot(placing.astype(bf16), scaled, preferred_element_type=f32)
    fold(flat, tall, ysend)
    for i in range(2, slots):
        gate_copy(i).start(priority=1)
        up_copy(i).start(priority=1)
    pl.semaphore_wait(barrier, EXPERTS + 2)

    def exchange(j):
        to = lax.rem(me + j, EXPERTS)
        return pltpu.make_async_remote_copy(
            src_ref=ysend.at[to], dst_ref=arr.at[me], send_sem=sent.at[0], recv_sem=a2a_recv.at[0],
            device_id=(p, to, t), device_id_type=MESH,
        )

    for j in (2, 3, 1):
        exchange(j).start()
    arr[me] = ysend[me]
    landed(arr.at[pl.ds(0, EXPERTS - 1)], a2a_recv.at[0])
    unfold(arr, tall, flat)

    def ss_copy(j):
        return pltpu.make_async_remote_copy(
            src_ref=ss_rows.at[t], dst_ref=ss_rows.at[t], send_sem=sent.at[1], recv_sem=sr_recv.at[0],
            device_id=(p, me, lax.rem(t + j, 4)), device_id_type=MESH,
        )

    def remote(src, dst, n, recv, i, to):
        return pltpu.make_async_remote_copy(
            src_ref=src, dst_ref=dst, send_sem=sent.at[n], recv_sem=recv.at[i],
            device_id=(p, me, to), device_id_type=MESH,
        )

    def at_half(c):
        return pl.ds(pl.multiple_of(c * half, half), half)

    def at_quarter(n):
        return pl.ds(pl.multiple_of(n * quarter, quarter), quarter)

    mine = own * 2 + xpos
    theirs = own * 2 + 1 - xpos

    def stage1(i):
        return remote(part.at[i, :, :, at_half(1 - own)], got1.at[i], 2, s1_recv, i, sibling)

    def stage2(i):
        return remote(half16.at[i, :, :, at_quarter(1 - xpos)], got2.at[i], 3, s2_recv, i, partner)

    def spread1(i):
        return remote(hid.at[i, :, at_quarter(mine)], hid.at[i, :, at_quarter(mine)], 4, h1_recv, i, partner)

    def spread2(i):
        return remote(hid.at[i, :, at_quarter(mine)], hid.at[i, :, at_quarter(mine)], 5, h2_recv, i, sibling)

    def spread3(i):
        return remote(hid.at[i, :, at_quarter(theirs)], hid.at[i, :, at_quarter(theirs)], 6, h2_recv, i, sibling)

    def exchange_squares():
        raw = flat[...] * (1.0 / gain[...].reshape(1, -1))
        ss_rows[t] = jnp.broadcast_to(jnp.sum(raw * raw, axis=1, keepdims=True), (rows, 128))
        for j in (1, 2, 3):
            ss_copy(j).start()

    def direct(i):
        return remote(hid.at[i, :, at_quarter(mine)], hid.at[i, :, at_quarter(mine)], 6, h2_recv, i, other)

    def multiply(i):
        s = i % slots
        pltpu.make_async_copy(lift_w.at[s], lift_w.at[s], lift_sem.at[s]).wait()
        part[i, 0] = jnp.dot(flat[...], lift_w[s, 0], preferred_element_type=f32).astype(bf16)
        part[i, 1] = jnp.dot(flat[...], lift_w[s, 1], preferred_element_type=f32).astype(bf16)
        stage1(i).start()
        when(i == 0, exchange_squares)

        if i + slots < chunks:
            gate_copy(i + slots).start(priority=1)
            up_copy(i + slots).start(priority=1)
        for n in (2 * (i - chunks + slots) - 1, 2 * (i - chunks + slots)):
            if 0 <= n < chunks:
                down_copy(n).start(priority=1)

    def add_core(b):
        stage1(b).wait_recv()
        for n in range(2):
            both = part[b, n, :, at_half(own)].astype(f32) + got1[b, n].astype(f32)
            half32[b, n] = both
            half16[b, n] = both.astype(bf16)
        stage2(b).start()

    def activate(c):
        def total():
            landed(ss_rows.at[pl.ds(0, 3)], sr_recv.at[0])
            landed(ss_rows.at[pl.ds(0, 3)], sent.at[1])
            ss_rows[t] = ss_rows[0] + ss_rows[1] + ss_rows[2] + ss_rows[3]

        when(c == 0, total)
        stage2(c).wait_recv()
        scale = lax.rsqrt(ss_rows[t][:, :1] / full_width + EPSILON)
        g = (half32[c, 0, :, at_quarter(xpos)] + got2[c, 0].astype(f32)) * scale
        u = (half32[c, 1, :, at_quarter(xpos)] + got2[c, 1].astype(f32)) * scale
        hid[c, :, at_quarter(mine)] = (g / (1.0 + jnp.exp(-g)) * u).astype(bf16)
        spread1(c).start()
        spread2(c).start()

        when(c >= chunks - DIRECT, lambda: direct(c).start())

    def hand_on(d):
        def pass_on():
            spread1(d).wait_recv()
            spread3(d).start()

        when(d < chunks - DIRECT, pass_on)

    def ready(e):
        when(e >= chunks - DIRECT, lambda: spread1(e).wait_recv())
        landed(hid.at[e, :, pl.ds(0, half)], h2_recv.at[e])
        down_copy(e).wait()

    def project(e):
        ready(e)
        acc[...] += jnp.dot(hid[e], down_w[e], preferred_element_type=f32)

    for i in range(chunks):
        multiply(i)
        when(i >= 1, lambda: add_core(i - 1))
        when(i >= 4, lambda: activate(i - 4))
        when(i >= 7, lambda: hand_on(i - 7))

    last = chunks - 1
    activate(last - 3)
    add_core(last)
    hand_on(last - 6)
    project(last - 7)
    hand_on(last - 5)
    activate(last - 2)
    project(last - 6)
    hand_on(last - 4)
    activate(last - 1)
    project(last - 5)
    hand_on(last - 3)
    activate(last)
    project(last - 4)
    hand_on(last - 2)
    project(last - 3)
    project(last - 2)
    project(last - 1)

    def give(b, j):
        to = lax.rem(me + j, EXPERTS)
        return pltpu.make_async_remote_copy(
            src_ref=ret_send.at[b, to], dst_ref=ret.at[b, me], send_sem=sent.at[7], recv_sem=rt_recv.at[b],
            device_id=(p, to, t), device_id_type=MESH,
        )

    wide = acc.shape[1] // blocks
    ready(last)
    for b in range(blocks):
        cols = slice(b * wide, (b + 1) * wide)
        acc[:, cols] += jnp.dot(hid[last], down_w[last, :, cols], preferred_element_type=f32)
        fold(acc.at[:, cols], rtall, ret_send.at[b])
        for j in (2, 3, 1):
            give(b, j).start()
        ret[b, me] = ret_send[b, me]

    landed(arr.at[pl.ds(0, EXPERTS - 1)], sent.at[0])
    landed(got1, sent.at[2])
    landed(got2, sent.at[3])
    for n in (4, 5, 6):
        landed(hid.at[:, :, pl.ds(0, quarter)], sent.at[n])
    for b in range(blocks):
        cols = slice(b * wide, (b + 1) * wide)
        landed(ret.at[b, pl.ds(0, EXPERTS - 1)], rt_recv.at[b])
        unfold(ret.at[b], rtall, flat.at[:, cols])
        moe = jnp.dot(mixt[...], flat[:, cols].astype(bf16), preferred_element_type=f32)
        out_ref[:, cols] = (resid[:, cols] + moe).astype(bf16)
    landed(ret.at[:, pl.ds(0, EXPERTS - 1)], sent.at[7])


def when(condition, run):
    if condition:
        run()


def landed(ref, sem):
    pltpu.make_async_copy(ref, ref, sem).wait()


def fold(flat, tall, out):
    for e in range(EXPERTS):
        for j in range(flat.shape[1] // 128):
            tall[e, j * CAP : (j + 1) * CAP] = flat[e * CAP : (e + 1) * CAP, j * 128 : (j + 1) * 128]
        out[e] = tall[e].astype(out.dtype)


def unfold(src, tall, flat):
    for e in range(EXPERTS):
        tall[e] = src[e].astype(tall.dtype)
        for j in range(flat.shape[1] // 128):
            flat[e * CAP : (e + 1) * CAP, j * 128 : (j + 1) * 128] = tall[e, j * CAP : (j + 1) * CAP]


DIRECT = 2


def fused(
    tokens, queries, new_kv, cache_kv, lengths, gain, gate_weight, up_weight, down_weight, routes, route_weights
):
    seqs, width_in = tokens.shape
    heads, hd = queries.shape[1:]
    ctx, kvh = cache_kv.shape[2:4]
    ff = gate_weight.shape[1]
    width = min(1024, ff)
    chunks = ff // width
    slots = min(5, chunks)
    rows = -(-EXPERTS * CAP // 8) * 8
    full_width = width_in * lax.axis_size("tensor")
    blocks = 2
    dims = (seqs, heads, heads // kvh, hd, ctx, kvh, full_width, chunks, width, slots, rows, blocks)
    low = -(-(width_in // 128 // blocks * CAP) // 8) * 8
    high = -(-(width_in // 128 * CAP) // 16) * 16
    half, quarter = width // 2, width // 4
    bf16, f32 = jnp.bfloat16, jnp.float32
    vm, dma = pltpu.VMEM, pltpu.SemaphoreType.DMA
    nk, nn = seqs * ctx * kvh, seqs * kvh
    scratch = [
        vm((1, seqs), jnp.int32), vm((2, seqs), jnp.int32),
        vm((seqs, width_in), bf16), vm((heads, seqs, hd), bf16), vm((2, nn, hd), bf16), vm((2, nk, hd), bf16),
        vm((width_in,), f32), vm((2, seqs), bf16), vm((seqs, width_in), f32), vm((seqs, rows), bf16),
        vm((EXPERTS, high, 128), bf16), vm((EXPERTS, high, 128), bf16),
        vm((4, rows, 128), f32), vm((rows, width_in), f32), vm((EXPERTS, high, 128), f32),
        vm((slots, 2, width_in, width), bf16), vm((chunks, width, width_in), bf16),
        vm((chunks, 2, rows, width), bf16), vm((chunks, 2, rows, half), bf16),
        vm((chunks, 2, rows, half), bf16), vm((chunks, 2, rows, half), f32),
        vm((chunks, 2, rows, quarter), bf16), vm((chunks, rows, width), bf16),
        vm((rows, width_in), f32), vm((EXPERTS, low, 128), f32),
        vm((blocks, EXPERTS, low, 128), bf16), vm((blocks, EXPERTS, low, 128), bf16),
        dma((8,)), dma((slots,)), dma((chunks,)), dma((8,)), dma((1,)), dma((1,)),
    ] + [dma((chunks,))] * 4 + [dma((blocks,))]
    anyspace = pl.BlockSpec(memory_space=pl.ANY)
    return pl.pallas_call(
        functools.partial(fused_kernel, dims),
        out_shape=pltpu.VMEM((seqs, width_in), bf16),
        in_specs=[anyspace] * 11,
        out_specs=pl.BlockSpec(memory_space=pltpu.VMEM),
        scratch_shapes=scratch,
        compiler_params=pltpu.CompilerParams(
            collective_id=0, has_side_effects=True, vmem_limit_bytes=66846720
        ),
    )(
        lengths.reshape(1, seqs), routes.T, tokens, jnp.transpose(queries, (1, 0, 2)), new_kv.reshape(2, nn, hd), cache_kv.reshape(2, nk, hd),
        gain, route_weights.T, gate_weight, up_weight, down_weight,
    )


def solution(mesh):
    in_specs = (
        P(("parts", "expert"), "tensor"),
        P(("parts", "expert"), "tensor", None),
        P(None, ("parts", "expert"), "tensor", None),
        P(None, ("parts", "expert"), None, "tensor", None),
        P(("parts", "expert")),
        P("tensor"),
        P("tensor", "expert"),
        P("tensor", "expert"),
        P("expert", "tensor"),
        P(("parts", "expert"), None),
        P(("parts", "expert"), None),
    )
    out_specs = P(("parts", "expert"), "tensor")
    square = mesh.shape["expert"] == EXPERTS and mesh.shape["tensor"] == 4

    def run(*args):
        wide = args[6].shape[1] >= 8 * 1024
        return (fused if square and wide else on_device)(*args)

    return jax.shard_map(
        run, mesh=mesh, in_specs=in_specs, out_specs=out_specs, check_vma=False
    )
```

```python
import functools
import math

import jax
import jax.numpy as jnp
from jax import lax
from jax.experimental import pallas as pl
from jax.experimental.pallas import tpu as pltpu
from jax.sharding import PartitionSpec as P

EXPERTS = 4
CAP = 9


EPSILON = 1e-05


def attend(queries, new_kv, cache_kv, lengths):
    sequences, head_count, head_size = queries.shape
    key_heads = new_kv.shape[2]
    groups = head_count // key_heads
    factor = 1.0 / math.sqrt(head_size)
    query_grp = queries.reshape(sequences, key_heads, groups, head_size)
    score_old = (
        jnp.einsum("skgd,spkd->skgp", query_grp, cache_kv[0], preferred_element_type=jnp.float32)
        * factor
    )
    score_new = (
        jnp.einsum("skgd,skd->skg", query_grp, new_kv[0], preferred_element_type=jnp.float32)
        * factor
    )
    position = jnp.arange(cache_kv.shape[2], dtype=jnp.int32)
    usable = (position[None, :] < lengths[:, None])[:, None, None, :]
    score_old = jnp.where(usable, score_old, -jnp.inf)
    largest = jnp.maximum(jnp.max(score_old, axis=3), score_new)
    weight_old = jnp.exp(score_old - largest[..., None])
    weight_new = jnp.exp(score_new - largest)
    denominator = jnp.sum(weight_old, axis=3) + weight_new
    prob_old = (weight_old / denominator[..., None]).astype(jnp.bfloat16)
    prob_new = (weight_new / denominator).astype(jnp.bfloat16)
    attended = jnp.einsum(
        "skgp,spkd->skgd", prob_old, cache_kv[1], preferred_element_type=jnp.float32
    )
    attended = (
        attended
        + prob_new.astype(jnp.float32)[..., None] * new_kv[1].astype(jnp.float32)[:, :, None, :]
    )
    return attended.reshape(sequences, head_count * head_size)


def expert_hidden(token_rows, gate_weight, up_weight, down_weight):
    gate_sum = jnp.dot(token_rows, gate_weight, preferred_element_type=jnp.float32)
    lift_sum = jnp.dot(token_rows, up_weight, preferred_element_type=jnp.float32)
    gate_sum, lift_sum = (
        lax.psum_scatter(gate_sum, "tensor", scatter_dimension=1, tiled=True),
        lax.psum_scatter(lift_sum, "tensor", scatter_dimension=1, tiled=True),
    )
    hidden = (jax.nn.silu(gate_sum) * lift_sum).astype(jnp.bfloat16)
    hidden = lax.all_gather(hidden, "tensor", axis=1, tiled=True)
    return jnp.dot(hidden, down_weight, preferred_element_type=jnp.float32)


def pack_slots(target, normed):
    slot_ids = jnp.arange(EXPERTS * CAP, dtype=jnp.int32)
    placing = (slot_ids[:, None, None] == target[None, :, :]).astype(jnp.float32)
    placing = jnp.sum(placing, axis=2).astype(jnp.bfloat16)
    packed = jnp.dot(placing, normed, preferred_element_type=jnp.float32).astype(jnp.bfloat16)
    return packed.reshape(EXPERTS, CAP, normed.shape[1])


def mix_slots(target, route_weights, per_slot):
    slot_ids = jnp.arange(EXPERTS * CAP, dtype=jnp.int32)
    mixing = jnp.where(
        slot_ids[None, None, :] == target[:, :, None],
        route_weights.astype(jnp.float32)[:, :, None],
        jnp.float32(0.0),
    )
    mixing = jnp.sum(mixing, axis=1)
    return jnp.dot(
        mixing, per_slot, precision=lax.Precision.HIGHEST, preferred_element_type=jnp.float32
    )


def on_device(
    tokens,
    queries,
    new_kv,
    cache_kv,
    lengths,
    gain,
    gate_weight,
    up_weight,
    down_weight,
    routes,
    route_weights,
):
    local_seqs, local_width = tokens.shape
    residual = tokens.astype(jnp.float32) + attend(queries, new_kv, cache_kv, lengths)
    full_width = local_width * lax.axis_size("tensor")
    squares = lax.psum(jnp.sum(residual * residual, axis=1), "tensor")
    normed = (residual * lax.rsqrt(squares[:, None] / full_width + EPSILON) * gain).astype(
        jnp.bfloat16
    )
    choosers = (routes[:, :, None] == jnp.arange(EXPERTS, dtype=jnp.int32)[None, None, :]).astype(
        jnp.int32
    )
    flat_choice = choosers.reshape(2 * local_seqs, EXPERTS)
    earlier = jnp.cumsum(flat_choice, axis=0) - flat_choice
    slot_index = jnp.sum(earlier * flat_choice, axis=1)
    target = (routes.reshape(-1) * CAP + slot_index).reshape(local_seqs, 2)
    devices = lax.axis_size("expert")
    per_expert = devices // EXPERTS
    packed = pack_slots(target, normed).reshape(EXPERTS, 1, CAP, local_width)
    outgoing = jnp.broadcast_to(packed, (EXPERTS, per_expert, CAP, local_width)).reshape(
        devices, CAP, local_width
    )
    arrived = lax.all_to_all(outgoing, "expert", split_axis=0, concat_axis=0, tiled=True)
    sources = arrived.shape[0]
    items = arrived.shape[1]
    produced = expert_hidden(
        arrived.reshape(sources * items, local_width), gate_weight, up_weight, down_weight
    )
    computed = produced.reshape(sources, items, local_width)
    returned = lax.all_to_all(computed, "expert", split_axis=0, concat_axis=0, tiled=True)
    per_slot = jnp.sum(returned.reshape(EXPERTS, per_expert, CAP, local_width), axis=1)
    moe_sum = mix_slots(target, route_weights, per_slot.reshape(EXPERTS * CAP, local_width))
    return (residual + moe_sum).astype(jnp.bfloat16)


MESH = pl.DeviceIdType.MESH


def fused_kernel(
    dims,
    lengths_hbm, routes_hbm,
    tokens_hbm, queries_hbm, new_hbm, cache_hbm, gain_hbm, mixw_hbm,
    gate_hbm, up_hbm, down_hbm,
    out_ref,
    lens, route, tok, qry, new, cache, gain, mixw, resid, mixt,
    ysend, arr, ss_rows, flat, tall,
    lift_w, down_w,
    part, got1, half16, half32, got2, hid, acc, rtall, ret_send, ret,
    in_sem, lift_sem, down_sem, sent, a2a_recv, sr_recv,
    s1_recv, s2_recv, h1_recv, h2_recv, rt_recv,
):
    seqs, heads, groups, hd, ctx, kvh, full_width, chunks, width, slots, rows, blocks = dims
    half, quarter = width // 2, width // 4
    p = lax.axis_index("parts")
    me = lax.axis_index("expert")
    t = lax.axis_index("tensor")
    core = lax.rem(t, 2)
    xpos = lax.div(t, 2)
    sibling = t + 1 - 2 * core
    partner = lax.rem(sibling + 2, 4)
    other = lax.rem(t + 2, 4)
    own = lax.rem(core + xpos, 2)
    f32, bf16 = jnp.float32, jnp.bfloat16

    barrier = pltpu.get_barrier_semaphore()
    for j in range(1, EXPERTS):
        pl.semaphore_signal(barrier, inc=1, device_id=(p, lax.rem(me + j, EXPERTS), t), device_id_type=MESH)
    for peer in (sibling, partner, other):
        pl.semaphore_signal(barrier, inc=1, device_id=(p, me, peer), device_id_type=MESH)

    small = [
        pltpu.make_async_copy(a, b, in_sem.at[n])
        for n, (a, b) in enumerate(
            [
                (queries_hbm, qry), (cache_hbm, cache), (new_hbm, new), (lengths_hbm, lens), (routes_hbm, route),
                (tokens_hbm, tok), (gain_hbm, gain), (mixw_hbm, mixw),
            ]
        )
    ]
    for cp in small:
        cp.start()

    def gate_copy(i):
        s = i % slots
        cols = pl.ds(i * width, width)
        return pltpu.make_async_copy(gate_hbm.at[:, cols], lift_w.at[s, 0], lift_sem.at[s, 0])

    def up_copy(i):
        s = i % slots
        cols = pl.ds(i * width, width)
        return pltpu.make_async_copy(up_hbm.at[:, cols], lift_w.at[s, 1], lift_sem.at[s, 1])

    def down_copy(i):
        rws = pl.ds(i * width, width)
        return pltpu.make_async_copy(down_hbm.at[rws, :], down_w.at[i], down_sem.at[i])

    for i in range(2):
        gate_copy(i).start(priority=1)
        up_copy(i).start(priority=1)
    tall[...] = jnp.zeros_like(tall)
    rtall[...] = jnp.zeros_like(rtall)
    acc[...] = jnp.zeros_like(acc)
    for cp in small:
        cp.wait()

    prow = lax.broadcasted_iota(jnp.int32, (rows, seqs), 0)
    expert_of = sum((prow >= e * CAP).astype(jnp.int32) for e in range(1, EXPERTS + 1))
    picks = [route[j : j + 1, :] == expert_of for j in range(2)]
    named = jnp.where(picks[0] | picks[1], f32(1.0), f32(0.0))
    earlier = lax.broadcasted_iota(jnp.int32, (seqs, seqs), 0) < lax.broadcasted_iota(jnp.int32, (seqs, seqs), 1)
    before = jnp.dot(
        named.astype(bf16), jnp.where(earlier, f32(1.0), f32(0.0)).astype(bf16), preferred_element_type=f32
    )
    slot_of = (prow - expert_of * CAP).astype(f32)
    placing = jnp.where(before == slot_of, named, f32(0.0))
    weights = mixw[...].astype(f32)
    mixing = placing * jnp.where(picks[0], weights[0:1], weights[1:2])
    same = lax.broadcasted_iota(jnp.int32, (seqs, seqs), 0) == lax.broadcasted_iota(jnp.int32, (seqs, seqs), 1)
    mixt[...] = lax.dot_general(
        jnp.where(same, f32(1.0), f32(0.0)).astype(bf16), mixing.astype(bf16), (((1,), (1,)), ((), ())),
        preferred_element_type=f32,
    ).astype(bf16)
    q = qry[...].reshape(heads * seqs, hd)
    factor = 1.0 / math.sqrt(hd)
    dn = (((1,), (1,)), ((), ()))
    nq, nk, nn = heads * seqs, seqs * ctx * kvh, seqs * kvh
    s_old = lax.dot_general(q, cache[0], dn, preferred_element_type=f32) * factor
    s_new = lax.dot_general(q, new[0], dn, preferred_element_type=f32) * factor
    kcol = lax.broadcasted_iota(jnp.int32, (1, nk), 1)
    owner = lax.broadcasted_iota(jnp.int32, (seqs, nk), 0)
    spread = lax.broadcasted_iota(jnp.int32, (seqs, nk), 1) // (ctx * kvh) == owner
    limit = jnp.dot(
        lens[...].astype(f32).astype(bf16), jnp.where(spread, f32(1.0), f32(0.0)).astype(bf16),
        preferred_element_type=f32,
    )
    kpos = (kcol // kvh) % ctx
    key_old = jnp.where(kpos.astype(f32) < limit, (kcol // (ctx * kvh)) * kvh + kcol % kvh, -1)
    key_new = lax.broadcasted_iota(jnp.int32, (1, nn), 1)
    qrow = lax.broadcasted_iota(jnp.int32, (nq, 1), 0)
    key_q = (qrow % seqs) * kvh + qrow // (seqs * groups)
    low = f32(-1e30)
    s_old = jnp.where(key_q == key_old, s_old, low)
    s_new = jnp.where(key_q == key_new, s_new, low)
    largest = jnp.maximum(jnp.max(s_old, axis=1, keepdims=True), jnp.max(s_new, axis=1, keepdims=True))
    w_old = jnp.exp(s_old - largest)
    w_new = jnp.exp(s_new - largest)
    den = jnp.sum(w_old, axis=1, keepdims=True) + jnp.sum(w_new, axis=1, keepdims=True)
    p_old = (w_old / den).astype(bf16)
    p_new = (w_new / den).astype(bf16)
    att = jnp.dot(p_old, cache[1], preferred_element_type=f32) + jnp.dot(
        p_new, new[1], preferred_element_type=f32
    )
    for h in range(heads):
        cols = slice(h * hd, (h + 1) * hd)
        piece = tok[:, cols].astype(f32) + att[h * seqs : (h + 1) * seqs]
        resid[:, cols] = piece
    scaled = (resid[...] * gain[...].reshape(1, -1)).astype(bf16)
    flat[...] = jnp.dot(placing.astype(bf16), scaled, preferred_element_type=f32)
    fold(flat, tall, ysend)
    for i in range(2, slots):
        gate_copy(i).start(priority=1)
        up_copy(i).start(priority=1)
    pl.semaphore_wait(barrier, EXPERTS + 2)

    def exchange(j):
        to = lax.rem(me + j, EXPERTS)
        return pltpu.make_async_remote_copy(
            src_ref=ysend.at[to], dst_ref=arr.at[me], send_sem=sent.at[0], recv_sem=a2a_recv.at[0],
            device_id=(p, to, t), device_id_type=MESH,
        )

    for j in (2, 3, 1):
        exchange(j).start()
    arr[me] = ysend[me]
    landed(arr.at[pl.ds(0, EXPERTS - 1)], a2a_recv.at[0])
    unfold(arr, tall, flat)

    def ss_copy(j):
        return pltpu.make_async_remote_copy(
            src_ref=ss_rows.at[t], dst_ref=ss_rows.at[t], send_sem=sent.at[1], recv_sem=sr_recv.at[0],
            device_id=(p, me, lax.rem(t + j, 4)), device_id_type=MESH,
        )

    def remote(src, dst, n, recv, i, to):
        return pltpu.make_async_remote_copy(
            src_ref=src, dst_ref=dst, send_sem=sent.at[n], recv_sem=recv.at[i],
            device_id=(p, me, to), device_id_type=MESH,
        )

    whole = rows - 8
    upper = lax.broadcasted_iota(jnp.int32, (8, width), 0) < 4

    last = chunks - 1

    def at_half(c):
        return pl.ds(pl.multiple_of(c * half, half), half)

    def at_quarter(n):
        return pl.ds(pl.multiple_of(n * quarter, quarter), quarter)

    mine = own * 2 + xpos
    theirs = own * 2 + 1 - xpos

    def stage1(i):
        return remote(part.at[i, :, at_half(1 - own)], got1.at[i], 2, s1_recv, i, sibling)

    def stage2(i):
        return remote(half16.at[i, :, at_quarter(1 - xpos)], got2.at[i], 3, s2_recv, i, partner)

    def spread1(i):
        return remote(hid.at[i, :, at_quarter(mine)], hid.at[i, :, at_quarter(mine)], 4, h1_recv, i, partner)

    def spread2(i):
        return remote(hid.at[i, :, at_quarter(mine)], hid.at[i, :, at_quarter(mine)], 5, h2_recv, i, sibling)

    def spread3(i):
        return remote(hid.at[i, :, at_quarter(theirs)], hid.at[i, :, at_quarter(theirs)], 6, h2_recv, i, sibling)

    def exchange_squares():
        raw = flat[...] * (1.0 / gain[...].reshape(1, -1))
        ss_rows[t] = jnp.broadcast_to(jnp.sum(raw * raw, axis=1, keepdims=True), (rows, 128))
        for j in (1, 2, 3):
            ss_copy(j).start()

    def direct(i):
        return remote(
            hid.at[i, :, at_quarter(mine)], hid.at[i, :, at_quarter(mine)], 6, h2_recv, chunks if i == last else i, other
        )

    def multiply(i):
        s = i % slots
        gate_copy(i).wait()
        if i < chunks - 2:
            up_copy(i).wait()
        g = jnp.dot(flat[...], lift_w[s, 0], preferred_element_type=f32)
        part[i, :whole] = g[:whole].astype(bf16)
        if i >= chunks - 2:
            up_copy(i).wait()
        u = jnp.dot(flat[...], lift_w[s, 1], preferred_element_type=f32)
        part[i, whole : 2 * whole] = u[:whole].astype(bf16)
        part[i, 2 * whole :] = jnp.where(upper, g[whole:], pltpu.roll(u[whole:], 4, 0)).astype(bf16)
        stage1(i).start()
        when(i == 0, exchange_squares)

        if i + slots < chunks:
            gate_copy(i + slots).start(priority=1)
            up_copy(i + slots).start(priority=1)
        for n in (2 * (i - chunks + slots) - 1, 2 * (i - chunks + slots)):
            if 0 <= n < chunks:
                down_copy(n).start(priority=1)

    def add_core(b):
        stage1(b).wait_recv()
        both = part[b, :, at_half(own)].astype(f32) + got1[b].astype(f32)
        half32[b] = both
        half16[b] = both.astype(bf16)
        stage2(b).start()

    def activate(c):
        def total():
            landed(ss_rows.at[pl.ds(0, 3)], sr_recv.at[0])
            landed(ss_rows.at[pl.ds(0, 3)], sent.at[1])
            ss_rows[t] = ss_rows[0] + ss_rows[1] + ss_rows[2] + ss_rows[3]

        when(c == 0, total)
        stage2(c).wait_recv()
        scale = lax.rsqrt(ss_rows[t][:, :1] / full_width + EPSILON)
        sums = half32[c, :, at_quarter(xpos)] + got2[c].astype(f32)
        ends = sums[2 * whole :]
        for place, g, u in (
            (slice(0, whole), sums[:whole], sums[whole : 2 * whole]), (slice(whole, rows), ends, pltpu.roll(ends, 4, 0)),
        ):
            g, u = g * scale[place], u * scale[place]
            hid[c, place, at_quarter(mine)] = (g / (1.0 + jnp.exp(-g)) * u).astype(bf16)
        spread1(c).start()
        spread2(c).start()

        when(c >= chunks - DIRECT, lambda: direct(c).start())

    def hand_on(d):
        def pass_on():
            spread1(d).wait_recv()
            spread3(d).start()

        when(d < chunks - DIRECT, pass_on)

    def ready(e):
        when(e >= chunks - DIRECT, lambda: spread1(e).wait_recv())
        landed(hid.at[e, :, pl.ds(0, half)], h2_recv.at[e])
        down_copy(e).wait()

    def project(e):
        ready(e)
        acc[...] += jnp.dot(hid[e], down_w[e], preferred_element_type=f32)

    for i in range(chunks):
        multiply(i)
        when(i >= 1, lambda: add_core(i - 1))
        when(i >= 4, lambda: activate(i - 4))
        when(i >= 7, lambda: hand_on(i - 7))

    activate(last - 3)
    add_core(last)
    hand_on(last - 6)
    project(last - 7)
    hand_on(last - 5)
    activate(last - 2)
    project(last - 6)
    hand_on(last - 4)
    activate(last - 1)
    project(last - 5)
    hand_on(last - 3)
    activate(last)
    project(last - 4)
    project(last - 3)
    project(last - 2)
    project(last - 1)

    def give(b, j):
        to = lax.rem(me + j, EXPERTS)
        return pltpu.make_async_remote_copy(
            src_ref=ret_send.at[b, to], dst_ref=ret.at[b, me], send_sem=sent.at[7], recv_sem=rt_recv.at[b],
            device_id=(p, to, t), device_id_type=MESH,
        )

    wide = acc.shape[1] // blocks

    def share(n, cols):
        return jnp.dot(hid[last, :, at_quarter(n)], down_w[last, at_quarter(n), cols], preferred_element_type=f32)

    down_copy(last).wait()
    spread2(last).wait_recv()
    acc[...] += share(xpos, slice(None)) + share(2 + xpos, slice(None))
    spread1(last).wait_recv()
    direct(last).wait_recv()
    for b in range(blocks):
        cols = slice(b * wide, (b + 1) * wide)
        acc[:, cols] += share(1 - xpos, cols) + share(3 - xpos, cols)
        fold(acc.at[:, cols], rtall, ret_send.at[b])
        for j in (2, 3, 1):
            give(b, j).start()
        ret[b, me] = ret_send[b, me]

    landed(arr.at[pl.ds(0, EXPERTS - 1)], sent.at[0])
    landed(got1, sent.at[2])
    landed(got2, sent.at[3])
    for n in (4, 5, 6):
        landed(hid.at[:, :, pl.ds(0, quarter)], sent.at[n])
    for b in range(blocks):
        cols = slice(b * wide, (b + 1) * wide)
        landed(ret.at[b, pl.ds(0, EXPERTS - 1)], rt_recv.at[b])
        unfold(ret.at[b], rtall, flat.at[:, cols])
        moe = jnp.dot(mixt[...], flat[:, cols].astype(bf16), preferred_element_type=f32)
        out_ref[:, cols] = (resid[:, cols] + moe).astype(bf16)
    landed(ret.at[:, pl.ds(0, EXPERTS - 1)], sent.at[7])


def when(condition, run):
    if condition:
        run()


def landed(ref, sem):
    pltpu.make_async_copy(ref, ref, sem).wait()


def fold(flat, tall, out):
    for e in range(EXPERTS):
        for j in range(flat.shape[1] // 128):
            tall[e, j * CAP : (j + 1) * CAP] = flat[e * CAP : (e + 1) * CAP, j * 128 : (j + 1) * 128]
        out[e] = tall[e].astype(out.dtype)


def unfold(src, tall, flat):
    for e in range(EXPERTS):
        tall[e] = src[e].astype(tall.dtype)
        for j in range(flat.shape[1] // 128):
            flat[e * CAP : (e + 1) * CAP, j * 128 : (j + 1) * 128] = tall[e, j * CAP : (j + 1) * CAP]


DIRECT = 3


def fused(
    tokens, queries, new_kv, cache_kv, lengths, gain, gate_weight, up_weight, down_weight, routes, route_weights
):
    seqs, width_in = tokens.shape
    heads, hd = queries.shape[1:]
    ctx, kvh = cache_kv.shape[2:4]
    ff = gate_weight.shape[1]
    width = min(1024, ff)
    chunks = ff // width
    slots = min(5, chunks)
    rows = -(-EXPERTS * CAP // 8) * 8
    dense = 2 * rows - 8
    full_width = width_in * lax.axis_size("tensor")
    blocks = 2
    dims = (seqs, heads, heads // kvh, hd, ctx, kvh, full_width, chunks, width, slots, rows, blocks)
    low = -(-(width_in // 128 // blocks * CAP) // 8) * 8
    high = -(-(width_in // 128 * CAP) // 16) * 16
    half, quarter = width // 2, width // 4
    bf16, f32 = jnp.bfloat16, jnp.float32
    vm, dma = pltpu.VMEM, pltpu.SemaphoreType.DMA
    nk, nn = seqs * ctx * kvh, seqs * kvh
    scratch = [
        vm((1, seqs), jnp.int32), vm((2, seqs), jnp.int32),
        vm((seqs, width_in), bf16), vm((heads, seqs, hd), bf16), vm((2, nn, hd), bf16), vm((2, nk, hd), bf16),
        vm((width_in,), f32), vm((2, seqs), bf16), vm((seqs, width_in), f32), vm((seqs, rows), bf16),
        vm((EXPERTS, high, 128), bf16), vm((EXPERTS, high, 128), bf16),
        vm((4, rows, 128), f32), vm((rows, width_in), f32), vm((EXPERTS, high, 128), f32),
        vm((slots, 2, width_in, width), bf16), vm((chunks, width, width_in), bf16),
        vm((chunks, dense, width), bf16), vm((chunks, dense, half), bf16),
        vm((chunks, dense, half), bf16), vm((chunks, dense, half), f32),
        vm((chunks, dense, quarter), bf16), vm((chunks, rows, width), bf16),
        vm((rows, width_in), f32), vm((EXPERTS, low, 128), f32),
        vm((blocks, EXPERTS, low, 128), bf16), vm((blocks, EXPERTS, low, 128), bf16),
        dma((8,)), dma((slots, 2)), dma((chunks,)), dma((8,)), dma((1,)), dma((1,)),
    ] + [dma((chunks,))] * 3 + [dma((chunks + 1,)), dma((blocks,))]
    anyspace = pl.BlockSpec(memory_space=pl.ANY)
    return pl.pallas_call(
        functools.partial(fused_kernel, dims),
        out_shape=pltpu.VMEM((seqs, width_in), bf16),
        in_specs=[anyspace] * 11,
        out_specs=pl.BlockSpec(memory_space=pltpu.VMEM),
        scratch_shapes=scratch,
        compiler_params=pltpu.CompilerParams(
            collective_id=0, has_side_effects=True, vmem_limit_bytes=66846720
        ),
    )(
        lengths.reshape(1, seqs), routes.T, tokens, jnp.transpose(queries, (1, 0, 2)), new_kv.reshape(2, nn, hd), cache_kv.reshape(2, nk, hd),
        gain, route_weights.T, gate_weight, up_weight, down_weight,
    )


def solution(mesh):
    in_specs = (
        P(("parts", "expert"), "tensor"),
        P(("parts", "expert"), "tensor", None),
        P(None, ("parts", "expert"), "tensor", None),
        P(None, ("parts", "expert"), None, "tensor", None),
        P(("parts", "expert")),
        P("tensor"),
        P("tensor", "expert"),
        P("tensor", "expert"),
        P("expert", "tensor"),
        P(("parts", "expert"), None),
        P(("parts", "expert"), None),
    )
    out_specs = P(("parts", "expert"), "tensor")
    square = mesh.shape["expert"] == EXPERTS and mesh.shape["tensor"] == 4

    def run(*args):
        wide = args[6].shape[1] >= 8 * 1024
        return (fused if square and wide else on_device)(*args)

    return jax.shard_map(
        run, mesh=mesh, in_specs=in_specs, out_specs=out_specs, check_vma=False
    )
```

```python
import functools
import math

import jax
import jax.numpy as jnp
from jax import lax
from jax.experimental import pallas as pl
from jax.experimental.pallas import tpu as pltpu
from jax.sharding import PartitionSpec as P

EXPERTS = 4
CAP = 9


EPSILON = 1e-05


def attend(queries, new_kv, cache_kv, lengths):
    sequences, head_count, head_size = queries.shape
    key_heads = new_kv.shape[2]
    groups = head_count // key_heads
    factor = 1.0 / math.sqrt(head_size)
    query_grp = queries.reshape(sequences, key_heads, groups, head_size)
    score_old = (
        jnp.einsum("skgd,spkd->skgp", query_grp, cache_kv[0], preferred_element_type=jnp.float32)
        * factor
    )
    score_new = (
        jnp.einsum("skgd,skd->skg", query_grp, new_kv[0], preferred_element_type=jnp.float32)
        * factor
    )
    position = jnp.arange(cache_kv.shape[2], dtype=jnp.int32)
    usable = (position[None, :] < lengths[:, None])[:, None, None, :]
    score_old = jnp.where(usable, score_old, -jnp.inf)
    largest = jnp.maximum(jnp.max(score_old, axis=3), score_new)
    weight_old = jnp.exp(score_old - largest[..., None])
    weight_new = jnp.exp(score_new - largest)
    denominator = jnp.sum(weight_old, axis=3) + weight_new
    prob_old = (weight_old / denominator[..., None]).astype(jnp.bfloat16)
    prob_new = (weight_new / denominator).astype(jnp.bfloat16)
    attended = jnp.einsum(
        "skgp,spkd->skgd", prob_old, cache_kv[1], preferred_element_type=jnp.float32
    )
    attended = (
        attended
        + prob_new.astype(jnp.float32)[..., None] * new_kv[1].astype(jnp.float32)[:, :, None, :]
    )
    return attended.reshape(sequences, head_count * head_size)


def expert_hidden(token_rows, gate_weight, up_weight, down_weight):
    gate_sum = jnp.dot(token_rows, gate_weight, preferred_element_type=jnp.float32)
    lift_sum = jnp.dot(token_rows, up_weight, preferred_element_type=jnp.float32)
    gate_sum, lift_sum = (
        lax.psum_scatter(gate_sum, "tensor", scatter_dimension=1, tiled=True),
        lax.psum_scatter(lift_sum, "tensor", scatter_dimension=1, tiled=True),
    )
    hidden = (jax.nn.silu(gate_sum) * lift_sum).astype(jnp.bfloat16)
    hidden = lax.all_gather(hidden, "tensor", axis=1, tiled=True)
    return jnp.dot(hidden, down_weight, preferred_element_type=jnp.float32)


def pack_slots(target, normed):
    slot_ids = jnp.arange(EXPERTS * CAP, dtype=jnp.int32)
    placing = (slot_ids[:, None, None] == target[None, :, :]).astype(jnp.float32)
    placing = jnp.sum(placing, axis=2).astype(jnp.bfloat16)
    packed = jnp.dot(placing, normed, preferred_element_type=jnp.float32).astype(jnp.bfloat16)
    return packed.reshape(EXPERTS, CAP, normed.shape[1])


def mix_slots(target, route_weights, per_slot):
    slot_ids = jnp.arange(EXPERTS * CAP, dtype=jnp.int32)
    mixing = jnp.where(
        slot_ids[None, None, :] == target[:, :, None],
        route_weights.astype(jnp.float32)[:, :, None],
        jnp.float32(0.0),
    )
    mixing = jnp.sum(mixing, axis=1)
    return jnp.dot(
        mixing, per_slot, precision=lax.Precision.HIGHEST, preferred_element_type=jnp.float32
    )


def on_device(
    tokens,
    queries,
    new_kv,
    cache_kv,
    lengths,
    gain,
    gate_weight,
    up_weight,
    down_weight,
    routes,
    route_weights,
):
    local_seqs, local_width = tokens.shape
    residual = tokens.astype(jnp.float32) + attend(queries, new_kv, cache_kv, lengths)
    full_width = local_width * lax.axis_size("tensor")
    squares = lax.psum(jnp.sum(residual * residual, axis=1), "tensor")
    normed = (residual * lax.rsqrt(squares[:, None] / full_width + EPSILON) * gain).astype(
        jnp.bfloat16
    )
    choosers = (routes[:, :, None] == jnp.arange(EXPERTS, dtype=jnp.int32)[None, None, :]).astype(
        jnp.int32
    )
    flat_choice = choosers.reshape(2 * local_seqs, EXPERTS)
    earlier = jnp.cumsum(flat_choice, axis=0) - flat_choice
    slot_index = jnp.sum(earlier * flat_choice, axis=1)
    target = (routes.reshape(-1) * CAP + slot_index).reshape(local_seqs, 2)
    devices = lax.axis_size("expert")
    per_expert = devices // EXPERTS
    packed = pack_slots(target, normed).reshape(EXPERTS, 1, CAP, local_width)
    outgoing = jnp.broadcast_to(packed, (EXPERTS, per_expert, CAP, local_width)).reshape(
        devices, CAP, local_width
    )
    arrived = lax.all_to_all(outgoing, "expert", split_axis=0, concat_axis=0, tiled=True)
    sources = arrived.shape[0]
    items = arrived.shape[1]
    produced = expert_hidden(
        arrived.reshape(sources * items, local_width), gate_weight, up_weight, down_weight
    )
    computed = produced.reshape(sources, items, local_width)
    returned = lax.all_to_all(computed, "expert", split_axis=0, concat_axis=0, tiled=True)
    per_slot = jnp.sum(returned.reshape(EXPERTS, per_expert, CAP, local_width), axis=1)
    moe_sum = mix_slots(target, route_weights, per_slot.reshape(EXPERTS * CAP, local_width))
    return (residual + moe_sum).astype(jnp.bfloat16)


MESH = pl.DeviceIdType.MESH


def fused_kernel(
    dims,
    lengths_hbm, routes_hbm,
    tokens_hbm, queries_hbm, new_hbm, cache_hbm, gain_hbm, mixw_hbm,
    gate_hbm, up_hbm, down_hbm,
    out_ref,
    lens, route, tok, qry, new, cache, gain, mixw, resid, mixt,
    ysend, arr, ss_rows, flat, tall,
    lift_w, down_w,
    part, got1, half16, half32, got2, hid, acc, rtall, ret_send, ret,
    in_sem, lift_sem, down_sem, sent, a2a_recv, sr_recv,
    s1_recv, s2_recv, h1_recv, h2_recv, rt_recv,
):
    seqs, heads, groups, hd, ctx, kvh, full_width, chunks, width, slots, rows, blocks = dims
    half, quarter = width // 2, width // 4
    p = lax.axis_index("parts")
    me = lax.axis_index("expert")
    t = lax.axis_index("tensor")
    core = lax.rem(t, 2)
    xpos = lax.div(t, 2)
    sibling = t + 1 - 2 * core
    partner = lax.rem(sibling + 2, 4)
    other = lax.rem(t + 2, 4)
    own = lax.rem(core + xpos, 2)
    f32, bf16 = jnp.float32, jnp.bfloat16

    barrier = pltpu.get_barrier_semaphore()
    for j in range(1, EXPERTS):
        pl.semaphore_signal(barrier, inc=1, device_id=(p, lax.rem(me + j, EXPERTS), t), device_id_type=MESH)
    for peer in (sibling, partner, other):
        pl.semaphore_signal(barrier, inc=1, device_id=(p, me, peer), device_id_type=MESH)

    small = [
        pltpu.make_async_copy(a, b, in_sem.at[n])
        for n, (a, b) in enumerate(
            [
                (queries_hbm, qry), (cache_hbm, cache), (new_hbm, new), (lengths_hbm, lens), (routes_hbm, route),
                (tokens_hbm, tok), (gain_hbm, gain), (mixw_hbm, mixw),
            ]
        )
    ]
    for cp in small:
        cp.start()

    def gate_copy(i):
        s = i % slots
        cols = pl.ds(i * width, width)
        return pltpu.make_async_copy(gate_hbm.at[:, cols], lift_w.at[s, 0], lift_sem.at[s, 0])

    def up_copy(i):
        s = i % slots
        cols = pl.ds(i * width, width)
        return pltpu.make_async_copy(up_hbm.at[:, cols], lift_w.at[s, 1], lift_sem.at[s, 1])

    def down_copy(i):
        rws = pl.ds(i * width, width)
        return pltpu.make_async_copy(down_hbm.at[rws, :], down_w.at[i], down_sem.at[i])

    for i in range(2):
        gate_copy(i).start(priority=1)
        up_copy(i).start(priority=1)
    tall[...] = jnp.zeros_like(tall)
    rtall[...] = jnp.zeros_like(rtall)
    acc[...] = jnp.zeros_like(acc)
    for cp in small:
        cp.wait()

    prow = lax.broadcasted_iota(jnp.int32, (rows, seqs), 0)
    expert_of = sum((prow >= e * CAP).astype(jnp.int32) for e in range(1, EXPERTS + 1))
    picks = [route[j : j + 1, :] == expert_of for j in range(2)]
    named = jnp.where(picks[0] | picks[1], f32(1.0), f32(0.0))
    earlier = lax.broadcasted_iota(jnp.int32, (seqs, seqs), 0) < lax.broadcasted_iota(jnp.int32, (seqs, seqs), 1)
    before = jnp.dot(
        named.astype(bf16), jnp.where(earlier, f32(1.0), f32(0.0)).astype(bf16), preferred_element_type=f32
    )
    slot_of = (prow - expert_of * CAP).astype(f32)
    placing = jnp.where(before == slot_of, named, f32(0.0))
    weights = mixw[...].astype(f32)
    mixing = placing * jnp.where(picks[0], weights[0:1], weights[1:2])
    same = lax.broadcasted_iota(jnp.int32, (seqs, seqs), 0) == lax.broadcasted_iota(jnp.int32, (seqs, seqs), 1)
    mixt[...] = lax.dot_general(
        jnp.where(same, f32(1.0), f32(0.0)).astype(bf16), mixing.astype(bf16), (((1,), (1,)), ((), ())),
        preferred_element_type=f32,
    ).astype(bf16)
    q = qry[...].reshape(heads * seqs, hd)
    factor = 1.0 / math.sqrt(hd)
    dn = (((1,), (1,)), ((), ()))
    nq, nk, nn = heads * seqs, seqs * ctx * kvh, seqs * kvh
    s_old = lax.dot_general(q, cache[0], dn, preferred_element_type=f32) * factor
    s_new = lax.dot_general(q, new[0], dn, preferred_element_type=f32) * factor
    kcol = lax.broadcasted_iota(jnp.int32, (1, nk), 1)
    owner = lax.broadcasted_iota(jnp.int32, (seqs, nk), 0)
    spread = lax.broadcasted_iota(jnp.int32, (seqs, nk), 1) // (ctx * kvh) == owner
    limit = jnp.dot(
        lens[...].astype(f32).astype(bf16), jnp.where(spread, f32(1.0), f32(0.0)).astype(bf16),
        preferred_element_type=f32,
    )
    kpos = (kcol // kvh) % ctx
    key_old = jnp.where(kpos.astype(f32) < limit, (kcol // (ctx * kvh)) * kvh + kcol % kvh, -1)
    key_new = lax.broadcasted_iota(jnp.int32, (1, nn), 1)
    qrow = lax.broadcasted_iota(jnp.int32, (nq, 1), 0)
    key_q = (qrow % seqs) * kvh + qrow // (seqs * groups)
    low = f32(-1e30)
    s_old = jnp.where(key_q == key_old, s_old, low)
    s_new = jnp.where(key_q == key_new, s_new, low)
    largest = jnp.maximum(jnp.max(s_old, axis=1, keepdims=True), jnp.max(s_new, axis=1, keepdims=True))
    w_old = jnp.exp(s_old - largest)
    w_new = jnp.exp(s_new - largest)
    den = jnp.sum(w_old, axis=1, keepdims=True) + jnp.sum(w_new, axis=1, keepdims=True)
    p_old = (w_old / den).astype(bf16)
    p_new = (w_new / den).astype(bf16)
    att = jnp.dot(p_old, cache[1], preferred_element_type=f32) + jnp.dot(
        p_new, new[1], preferred_element_type=f32
    )
    for h in range(heads):
        cols = slice(h * hd, (h + 1) * hd)
        piece = tok[:, cols].astype(f32) + att[h * seqs : (h + 1) * seqs]
        resid[:, cols] = piece
    scaled = (resid[...] * gain[...].reshape(1, -1)).astype(bf16)
    flat[...] = jnp.dot(placing.astype(bf16), scaled, preferred_element_type=f32)
    fold(flat, tall, ysend)
    for i in range(2, slots):
        gate_copy(i).start(priority=1)
        up_copy(i).start(priority=1)
    pl.semaphore_wait(barrier, EXPERTS + 2)

    def exchange(j):
        to = lax.rem(me + j, EXPERTS)
        return pltpu.make_async_remote_copy(
            src_ref=ysend.at[to], dst_ref=arr.at[me], send_sem=sent.at[0], recv_sem=a2a_recv.at[0],
            device_id=(p, to, t), device_id_type=MESH,
        )

    for j in (2, 3, 1):
        exchange(j).start()
    arr[me] = ysend[me]
    landed(arr.at[pl.ds(0, EXPERTS - 1)], a2a_recv.at[0])
    unfold(arr, tall, flat)

    def ss_copy(j):
        return pltpu.make_async_remote_copy(
            src_ref=ss_rows.at[t], dst_ref=ss_rows.at[t], send_sem=sent.at[1], recv_sem=sr_recv.at[0],
            device_id=(p, me, lax.rem(t + j, 4)), device_id_type=MESH,
        )

    def remote(src, dst, n, recv, i, to):
        return pltpu.make_async_remote_copy(
            src_ref=src, dst_ref=dst, send_sem=sent.at[n], recv_sem=recv.at[i],
            device_id=(p, me, to), device_id_type=MESH,
        )

    whole = rows - 8
    upper = lax.broadcasted_iota(jnp.int32, (8, width), 0) < 4

    last = chunks - 1

    def at_half(c):
        return pl.ds(pl.multiple_of(c * half, half), half)

    def at_quarter(n):
        return pl.ds(pl.multiple_of(n * quarter, quarter), quarter)

    mine = own * 2 + xpos
    theirs = own * 2 + 1 - xpos

    def stage1(i):
        return remote(part.at[i, :, at_half(1 - own)], got1.at[i], 2, s1_recv, i, sibling)

    def stage2(i):
        return remote(half16.at[i, :, at_quarter(1 - xpos)], got2.at[i], 3, s2_recv, i, partner)

    def spread1(i):
        return remote(hid.at[i, :, at_quarter(mine)], hid.at[i, :, at_quarter(mine)], 4, h1_recv, i, partner)

    def spread2(i):
        return remote(hid.at[i, :, at_quarter(mine)], hid.at[i, :, at_quarter(mine)], 5, h2_recv, i, sibling)

    def spread3(i):
        return remote(hid.at[i, :, at_quarter(theirs)], hid.at[i, :, at_quarter(theirs)], 6, h2_recv, i, sibling)

    def exchange_squares():
        raw = flat[...] * (1.0 / gain[...].reshape(1, -1))
        ss_rows[t] = jnp.broadcast_to(jnp.sum(raw * raw, axis=1, keepdims=True), (rows, 128))
        for j in (1, 2, 3):
            ss_copy(j).start()

    def direct(i):
        return remote(
            hid.at[i, :, at_quarter(mine)], hid.at[i, :, at_quarter(mine)], 6, h2_recv, chunks if i == last else i, other
        )

    def multiply(i):
        s = i % slots
        gate_copy(i).wait()
        if i < chunks - 3:
            up_copy(i).wait()
        g = jnp.dot(flat[...], lift_w[s, 0], preferred_element_type=f32)
        part[i, :whole] = g[:whole].astype(bf16)
        if i >= chunks - 3:
            up_copy(i).wait()
        u = jnp.dot(flat[...], lift_w[s, 1], preferred_element_type=f32)
        part[i, whole : 2 * whole] = u[:whole].astype(bf16)
        part[i, 2 * whole :] = jnp.where(upper, g[whole:], pltpu.roll(u[whole:], 4, 0)).astype(bf16)
        stage1(i).start()
        when(i == 0, exchange_squares)

        if i + slots < chunks:
            gate_copy(i + slots).start(priority=1)
            up_copy(i + slots).start(priority=1)
        for n in (2 * (i - chunks + slots) - 1, 2 * (i - chunks + slots)):
            if 0 <= n < chunks:
                down_copy(n).start(priority=1)

    def add_core(b):
        stage1(b).wait_recv()
        both = part[b, :, at_half(own)].astype(f32) + got1[b].astype(f32)
        half32[b] = both
        half16[b] = both.astype(bf16)
        stage2(b).start()

    def activate(c):
        def total():
            landed(ss_rows.at[pl.ds(0, 3)], sr_recv.at[0])
            landed(ss_rows.at[pl.ds(0, 3)], sent.at[1])
            ss_rows[t] = ss_rows[0] + ss_rows[1] + ss_rows[2] + ss_rows[3]

        when(c == 0, total)
        stage2(c).wait_recv()
        scale = lax.rsqrt(ss_rows[t][:, :1] / full_width + EPSILON)
        sums = half32[c, :, at_quarter(xpos)] + got2[c].astype(f32)
        ends = sums[2 * whole :]
        for place, g, u in (
            (slice(0, whole), sums[:whole], sums[whole : 2 * whole]), (slice(whole, rows), ends, pltpu.roll(ends, 4, 0)),
        ):
            g, u = g * scale[place], u * scale[place]
            hid[c, place, at_quarter(mine)] = (g / (1.0 + jnp.exp(-g)) * u).astype(bf16)
        spread1(c).start()
        spread2(c).start()

        when(c >= chunks - DIRECT, lambda: direct(c).start())

    def hand_on(d):
        def pass_on():
            spread1(d).wait_recv()
            spread3(d).start()

        when(d < chunks - DIRECT, pass_on)

    def ready(e):
        when(e >= chunks - DIRECT, lambda: spread1(e).wait_recv())
        landed(hid.at[e, :, pl.ds(0, half)], h2_recv.at[e])
        down_copy(e).wait()

    def project(e):
        ready(e)
        acc[...] += jnp.dot(hid[e], down_w[e], preferred_element_type=f32)

    for i in range(chunks):
        multiply(i)
        when(i >= 1, lambda: add_core(i - 1))
        when(i >= 4, lambda: activate(i - 4))
        when(i >= 7, lambda: hand_on(i - 7))

    activate(last - 3)
    add_core(last)
    hand_on(last - 6)
    project(last - 7)
    hand_on(last - 5)
    activate(last - 2)
    project(last - 6)
    hand_on(last - 4)
    activate(last - 1)
    project(last - 5)
    hand_on(last - 3)
    activate(last)
    project(last - 4)
    project(last - 3)
    project(last - 2)
    project(last - 1)

    def give(b, j):
        to = lax.rem(me + j, EXPERTS)
        return pltpu.make_async_remote_copy(
            src_ref=ret_send.at[b, to], dst_ref=ret.at[b, me], send_sem=sent.at[7], recv_sem=rt_recv.at[b],
            device_id=(p, to, t), device_id_type=MESH,
        )

    wide = acc.shape[1] // blocks

    def share(n, cols):
        return jnp.dot(hid[last, :, at_quarter(n)], down_w[last, at_quarter(n), cols], preferred_element_type=f32)

    down_copy(last).wait()
    spread2(last).wait_recv()
    acc[...] += share(xpos, slice(None)) + share(2 + xpos, slice(None))
    spread1(last).wait_recv()
    direct(last).wait_recv()
    for b in range(blocks):
        cols = slice(b * wide, (b + 1) * wide)
        acc[:, cols] += share(1 - xpos, cols) + share(3 - xpos, cols)
        fold(acc.at[:, cols], rtall, ret_send.at[b])
        for j in (2, 3, 1):
            give(b, j).start()
        ret[b, me] = ret_send[b, me]

    landed(arr.at[pl.ds(0, EXPERTS - 1)], sent.at[0])
    landed(got1, sent.at[2])
    landed(got2, sent.at[3])
    for n in (4, 5, 6):
        landed(hid.at[:, :, pl.ds(0, quarter)], sent.at[n])
    for b in range(blocks):
        cols = slice(b * wide, (b + 1) * wide)
        landed(ret.at[b, pl.ds(0, EXPERTS - 1)], rt_recv.at[b])
        unfold(ret.at[b], rtall, flat.at[:, cols])
        moe = jnp.dot(mixt[...], flat[:, cols].astype(bf16), preferred_element_type=f32)
        out_ref[:, cols] = (resid[:, cols] + moe).astype(bf16)
    landed(ret.at[:, pl.ds(0, EXPERTS - 1)], sent.at[7])


def when(condition, run):
    if condition:
        run()


def landed(ref, sem):
    pltpu.make_async_copy(ref, ref, sem).wait()


def fold(flat, tall, out):
    for e in range(EXPERTS):
        for j in range(flat.shape[1] // 128):
            tall[e, j * CAP : (j + 1) * CAP] = flat[e * CAP : (e + 1) * CAP, j * 128 : (j + 1) * 128]
        out[e] = tall[e].astype(out.dtype)


def unfold(src, tall, flat):
    for e in range(EXPERTS):
        tall[e] = src[e].astype(tall.dtype)
        for j in range(flat.shape[1] // 128):
            flat[e * CAP : (e + 1) * CAP, j * 128 : (j + 1) * 128] = tall[e, j * CAP : (j + 1) * CAP]


DIRECT = 3


def fused(
    tokens, queries, new_kv, cache_kv, lengths, gain, gate_weight, up_weight, down_weight, routes, route_weights
):
    seqs, width_in = tokens.shape
    heads, hd = queries.shape[1:]
    ctx, kvh = cache_kv.shape[2:4]
    ff = gate_weight.shape[1]
    width = min(1024, ff)
    chunks = ff // width
    slots = min(5, chunks)
    rows = -(-EXPERTS * CAP // 8) * 8
    dense = 2 * rows - 8
    full_width = width_in * lax.axis_size("tensor")
    blocks = 2
    dims = (seqs, heads, heads // kvh, hd, ctx, kvh, full_width, chunks, width, slots, rows, blocks)
    low = -(-(width_in // 128 // blocks * CAP) // 8) * 8
    high = -(-(width_in // 128 * CAP) // 16) * 16
    half, quarter = width // 2, width // 4
    bf16, f32 = jnp.bfloat16, jnp.float32
    vm, dma = pltpu.VMEM, pltpu.SemaphoreType.DMA
    nk, nn = seqs * ctx * kvh, seqs * kvh
    scratch = [
        vm((1, seqs), jnp.int32), vm((2, seqs), jnp.int32),
        vm((seqs, width_in), bf16), vm((heads, seqs, hd), bf16), vm((2, nn, hd), bf16), vm((2, nk, hd), bf16),
        vm((width_in,), f32), vm((2, seqs), bf16), vm((seqs, width_in), f32), vm((seqs, rows), bf16),
        vm((EXPERTS, high, 128), bf16), vm((EXPERTS, high, 128), bf16),
        vm((4, rows, 128), f32), vm((rows, width_in), f32), vm((EXPERTS, high, 128), f32),
        vm((slots, 2, width_in, width), bf16), vm((chunks, width, width_in), bf16),
        vm((chunks, dense, width), bf16), vm((chunks, dense, half), bf16),
        vm((chunks, dense, half), bf16), vm((chunks, dense, half), f32),
        vm((chunks, dense, quarter), bf16), vm((chunks, rows, width), bf16),
        vm((rows, width_in), f32), vm((EXPERTS, low, 128), f32),
        vm((blocks, EXPERTS, low, 128), bf16), vm((blocks, EXPERTS, low, 128), bf16),
        dma((8,)), dma((slots, 2)), dma((chunks,)), dma((8,)), dma((1,)), dma((1,)),
    ] + [dma((chunks,))] * 3 + [dma((chunks + 1,)), dma((blocks,))]
    anyspace = pl.BlockSpec(memory_space=pl.ANY)
    return pl.pallas_call(
        functools.partial(fused_kernel, dims),
        out_shape=pltpu.VMEM((seqs, width_in), bf16),
        in_specs=[anyspace] * 11,
        out_specs=pl.BlockSpec(memory_space=pltpu.VMEM),
        scratch_shapes=scratch,
        compiler_params=pltpu.CompilerParams(
            collective_id=0, has_side_effects=True, vmem_limit_bytes=66846720
        ),
    )(
        lengths.reshape(1, seqs), routes.T, tokens, jnp.transpose(queries, (1, 0, 2)), new_kv.reshape(2, nn, hd), cache_kv.reshape(2, nk, hd),
        gain, route_weights.T, gate_weight, up_weight, down_weight,
    )


def solution(mesh):
    in_specs = (
        P(("parts", "expert"), "tensor"),
        P(("parts", "expert"), "tensor", None),
        P(None, ("parts", "expert"), "tensor", None),
        P(None, ("parts", "expert"), None, "tensor", None),
        P(("parts", "expert")),
        P("tensor"),
        P("tensor", "expert"),
        P("tensor", "expert"),
        P("expert", "tensor"),
        P(("parts", "expert"), None),
        P(("parts", "expert"), None),
    )
    out_specs = P(("parts", "expert"), "tensor")
    square = mesh.shape["expert"] == EXPERTS and mesh.shape["tensor"] == 4

    def run(*args):
        wide = args[6].shape[1] >= 8 * 1024
        return (fused if square and wide else on_device)(*args)

    return jax.shard_map(
        run, mesh=mesh, in_specs=in_specs, out_specs=out_specs, check_vma=False
    )
```
